128 devices in a mesh: dev: 128 (over z, x, y, core).
Axes of the slice: x: 4, y: 4, z: 4, core: 2. Of those that a mesh axis runs over, the one named last changes fastest.
Arguments:
- state: float32 [2, 4194304], P(None, 'dev'), as said below
- angles: float32 [22, 3], replicated, may hold values from -3.140625 to 3.140625
- sample_high: int32 [1048576, 1], P('dev'), may hold values from 0 to 127; in each aligned block of 8192 rows (0 to 8191, 8192 to 16383, ...) at most 256 rows name the same one
- sample_low: int32 [1048576], P('dev'), may hold values from 0 to 32767
- marginal_qubits: int32 [10], replicated, may hold values from 0 to 21, as said below
Outputs:
- sample_probs: float32 [1048576], P('dev')
- histogram: float32 [1024], P('dev')
- fidelity: float32 [], replicated
The draws below stay inside these ranges and needn't reach their ends.
Inputs may be any that keep to these rules, and one draw needn't show every extreme that they name: The state is unit noise times a product over qubits of factors between exp(-0.2) and exp(0.2). `marginal_qubits`: 10 different qubit numbers. `sample_high`: among the rows of one device no value occurs more than 256 times, and in some devices one value occurs exactly 256 times.
All inputs are finite; a program needn't handle non-finite values.
Results may differ from the reference program's by a relative error of at most 0.00075.
Values sent between devices are 32-bit elements.
A program may use at most 64 MiB of HBM per device.

```python
import math
import jax
import jax.numpy as jnp
import numpy as np

QUBITS = 22
AMPS_DEV = 32768
AMPS = 4194304
SAMP_DEV = 8192
SAMPLES = 1048576
OWNERS = 128
CAP = 256
MARG = 10
MARG_BINS = 1024


def draw_state(key, part):
    key_envelope = jax.random.fold_in(key, 11)
    key_noise = jax.random.fold_in(key, 12)
    factors = jax.random.uniform(key_envelope, (QUBITS,), jnp.float32, -0.15, 0.15)
    noise = jax.random.normal(key_noise, (2, AMPS), jnp.float32)
    index = jnp.arange(AMPS, dtype=jnp.int32)
    exponent = jnp.zeros((AMPS,), jnp.float32)
    for qubit in range(QUBITS):
        exponent = exponent + factors[qubit] * (index >> qubit & 1).astype(jnp.float32)
    return noise * jnp.exp(exponent)[None, :]


def draw_marginal_qubits(key, part):
    return jax.random.permutation(jax.random.fold_in(key, 21), QUBITS)[:MARG].astype(jnp.int32)


def set_ends(values, rng, least, top_value):
    spot = [jax.random.randint(jax.random.fold_in(rng, axis), (), 0, length) for axis, length in enumerate(values.shape)]
    widest = values.shape.index(max(values.shape))
    neighbour = spot[:widest] + [(spot[widest] + 1) % values.shape[widest]] + spot[widest + 1:]
    return values.at[tuple(spot)].set(least).at[tuple(neighbour)].set(top_value)


def rank_bounds(amount, lean):
    loads = [(1 << 20) // math.isqrt(standing ** lean) + 1 for standing in range(1, amount + 1)]
    deviation = 1 + sum(loads) // (1 << 30)
    return np.cumsum(np.array([max(1, weight // deviation) for weight in loads]))


def ranked_ids(stream_key, shape, number_of, skew):
    grid = rank_bounds(number_of, skew)
    pick = jax.random.randint(jax.random.fold_in(stream_key, 1), shape, 0, int(grid[number_of - 1]))
    standing = jnp.searchsorted(jnp.asarray(grid, jnp.int32), pick, side="right")
    return jax.random.permutation(jax.random.fold_in(stream_key, 2), number_of)[standing].astype(jnp.int32)


def assign_block(stream_key, own, number, rows, count, top, bound, skew):
    ranking = jax.random.permutation(stream_key, count)
    heavy_load, ordinary = portions_of(count, rows * top, bound, skew, True), portions_of(count, rows * top, bound, skew, False)
    places = jnp.arange(count)

    def named(lengths, offset_by):
        used = int((lengths > 0).sum())
        fixed = max(1, used // 4)
        passed = fixed + (places - fixed + offset_by * (used - fixed)) % max(1, count - fixed)
        return jnp.zeros((count,), jnp.int32).at[ranking[jnp.where(places < fixed, places, passed)]].set(jnp.asarray(lengths, jnp.int32))

    lengths = jnp.where(number % 4 == 0, named(heavy_load, number // 4), named(ordinary, number - number // 4 - 1))
    mixed = jax.random.permutation(jax.random.fold_in(own, 3), count)
    source_of, taker = mixed[0:count // 2 * 2:2], mixed[1:count // 2 * 2:2]
    margin = jnp.minimum(lengths[source_of] - 1, bound - lengths[taker]) // 2
    margin = jnp.where((source_of == ranking[0]) | (taker == ranking[0]) | (lengths[taker] == 0), 0, jnp.maximum(margin, 0))
    passed = jax.random.randint(jax.random.fold_in(own, 4), (count // 2,), 0, 1 << 20) % (margin + 1)
    lengths = lengths.at[source_of].add(-passed).at[taker].add(passed)
    items = jnp.searchsorted(jnp.cumsum(lengths), jnp.arange(rows * top), side="right").astype(jnp.int32)
    grid = items.reshape(top, rows).T
    grid = grid[jax.random.permutation(jax.random.fold_in(own, 1), rows)]
    offset_by = jax.random.randint(jax.random.fold_in(own, 2), (rows, 1), 0, top)
    return jnp.take_along_axis(grid, (jnp.arange(top)[None, :] + offset_by) % top, axis=1)


def portions_of(count, total, bound, skew, full):
    loads = [(1 << 20) // math.isqrt(grade ** skew) + 1 for grade in range(1, count + 1)]
    largest = bound if full else min(bound, max(-(-total // count), total * loads[0] // sum(loads)))
    least = 1 if total - largest >= count - 1 else 0
    counts, spare = [largest] + [least] * (count - 1), total - largest - least * (count - 1)
    while spare > 0:
        candidates = [i for i in range(1, count) if counts[i] < largest] or [i for i in range(1, count) if counts[i] < bound]
        whole, left = sum([loads[i] for i in candidates]), spare
        for i in candidates:
            more = min(bound - counts[i], max(1, left * loads[i] // whole), spare)
            counts[i] = counts[i] + more
            spare = spare - more
    return np.array(counts)


def setup_inputs(seed: int = 0) -> dict:
    keys = jax.random.split(jax.random.key(seed), 6)
    state = draw_state(jax.random.fold_in(keys[5], 71), 0)
    angles = jnp.clip(jax.random.uniform(keys[1], (QUBITS, 3), jnp.float32, -3.140625, 3.140625), -3.140625, 3.140625)
    sample_high_keys = jax.random.split(jax.random.fold_in(keys[2], 1), SAMPLES // SAMP_DEV)
    sample_high_turns = jax.random.permutation(jax.random.fold_in(keys[2], 3), SAMPLES // SAMP_DEV)
    sample_high = jax.vmap(lambda own, number: assign_block(jax.random.fold_in(keys[2], 2), own, number, SAMP_DEV, OWNERS, 1, CAP, 2))(sample_high_keys, sample_high_turns).reshape((SAMPLES, 1))
    sample_low = set_ends(ranked_ids(keys[3], (SAMPLES,), AMPS_DEV, 2), jax.random.fold_in(keys[3], 3), 0, AMPS_DEV - 1).astype(jnp.int32)
    marginal_qubits = draw_marginal_qubits(jax.random.fold_in(keys[5], 71), 0)
    return {"state": state, "angles": angles, "sample_high": sample_high, "sample_low": sample_low, "marginal_qubits": marginal_qubits}


def gate_parts(angles):
    theta = angles[:, 0]
    first = angles[:, 1]
    second = angles[:, 2]
    cosine = jnp.cos(theta)
    sine = jnp.sin(theta)
    zeros = jnp.zeros_like(cosine)
    real_part = jnp.stack([jnp.stack([cosine, -jnp.cos(second) * sine], -1),
                           jnp.stack([jnp.cos(first) * sine, jnp.cos(first + second) * cosine], -1)], -2)
    imag_part = jnp.stack([jnp.stack([zeros, -jnp.sin(second) * sine], -1),
                           jnp.stack([jnp.sin(first) * sine, jnp.sin(first + second) * cosine], -1)], -2)
    return real_part, imag_part


def reference(state, angles, sample_high, sample_low, marginal_qubits):
    gate_real, gate_imag = gate_parts(angles)
    real_part = state[0]
    imag_part = state[1]
    for qubit in range(QUBITS):
        shape = (AMPS // (2 * 2 ** qubit), 2, 2 ** qubit)
        field_real = real_part.reshape(shape)
        field_imag = imag_part.reshape(shape)
        zero_real, zero_imag = field_real[:, 0], field_imag[:, 0]
        one_real, one_imag = field_real[:, 1], field_imag[:, 1]
        outputs_real = []
        outputs_imag = []
        for row in range(2):
            ar, ai = gate_real[qubit, row, 0], gate_imag[qubit, row, 0]
            br, bi = gate_real[qubit, row, 1], gate_imag[qubit, row, 1]
            outputs_real.append(ar * zero_real - ai * zero_imag + br * one_real - bi * one_imag)
            outputs_imag.append(ar * zero_imag + ai * zero_real + br * one_imag + bi * one_real)
        real_part = jnp.stack(outputs_real, 1).reshape(AMPS)
        imag_part = jnp.stack(outputs_imag, 1).reshape(AMPS)
    weight = real_part * real_part + imag_part * imag_part
    norm = jnp.sum(weight)
    bitstring = sample_high[:, 0] * AMPS_DEV + sample_low
    sample_probs = AMPS * (jnp.take(weight, bitstring) / norm)
    fidelity = jnp.mean(sample_probs) - 1.0
    index = jnp.arange(AMPS, dtype=jnp.int32)
    bins = jnp.zeros((AMPS,), jnp.int32)
    for place in range(MARG):
        bins = bins + (((index >> marginal_qubits[place]) & 1) << place)
    totals = jax.ops.segment_sum(weight, bins, num_segments=MARG_BINS)
    histogram = MARG_BINS * (totals / norm)
    return sample_probs, histogram, fidelity
```

```python
import functools

import jax
import jax.numpy as jnp
from jax import lax
from jax.experimental import pallas as pl
from jax.experimental.pallas import tpu as pltpu
from jax.sharding import PartitionSpec as P

N = 128
MESH = pl.DeviceIdType.MESH
F32 = jnp.float32
BF16 = jnp.bfloat16
I32 = jnp.int32


def iota(shape, dim):
    return lax.broadcasted_iota(I32, shape, dim)


def dot(a, b):
    return jnp.dot(a, b, preferred_element_type=F32)


def split(x):
    high = x.astype(BF16)
    low = (x - high.astype(F32)).astype(BF16)
    return high, low


def dot3(a, b):
    a_high, a_low = split(a)
    b_high, b_low = split(b)
    return dot(a_high, b_high) + (dot(a_high, b_low) + dot(a_low, b_high))


def complex_mul(a, b):
    return (a[0] * b[0] - a[1] * b[1], a[0] * b[1] + a[1] * b[0])


def gate_entries(angles):
    rows = angles.shape[0]
    lane = iota((rows, 128), 1)
    theta, first, second = (
        jnp.broadcast_to(angles[:, k : k + 1], (rows, 128)) for k in range(3)
    )
    packed = jnp.where(
        lane == 0, theta, jnp.where(lane == 1, first, jnp.where(lane == 2, second, first + second))
    )
    sines, cosines = jnp.sin(packed), jnp.cos(packed)

    def column(x, k):
        return jnp.broadcast_to(x[:, k : k + 1], (rows, 128))

    ct, st = column(cosines, 0), column(sines, 0)
    return [
        (ct, jnp.zeros_like(ct)),
        (-column(cosines, 2) * st, -column(sines, 2) * st),
        (column(cosines, 1) * st, column(sines, 1) * st),
        (column(cosines, 3) * ct, column(sines, 3) * ct),
    ]


def kron_matrix(entry, qubits, transposed):
    size = 2 ** len(qubits)
    lane, sub = iota((8, size), 1), iota((8, size), 0)

    def factor_rows(place, qubit):
        bit = (lane >> place) & 1 == 1

        def choose(zero, one):
            return tuple(
                jnp.where(bit, entry(one, part, qubit, size), entry(zero, part, qubit, size))
                for part in range(2)
            )

        if transposed:
            return choose(0, 2), choose(1, 3)
        return choose(0, 1), choose(2, 3)

    mat = None
    for place, qubit in enumerate(qubits):
        row_zero, row_one = factor_rows(place, qubit)
        if place < 3:
            bit = (sub >> place) & 1 == 1
            factor = tuple(jnp.where(bit, row_one[k], row_zero[k]) for k in range(2))
            mat = factor if mat is None else complex_mul(mat, factor)
        else:
            count = mat[0].shape[0] // 8
            halves = []
            for row in (row_zero, row_one):
                wide = tuple(jnp.concatenate([x] * count, axis=0) for x in row)
                halves.append(complex_mul(mat, wide))
            mat = tuple(jnp.concatenate([halves[0][k], halves[1][k]], axis=0) for k in range(2))
    return mat


def select_rows(values, bits):
    for bit in bits:
        half = values.shape[0] // 2
        values = jnp.where(bit, values[half:], values[:half])
    return values


def pick_sublane(values, index):
    hit = iota(values.shape, 0) == index
    return jnp.sum(jnp.where(hit, values, 0.0), axis=0, keepdims=True)


def bit_of(x, place):
    return (x >> place) & 1 == 1


def kernel(
    state_ref, angles_ref, high_ref, low_ref, marg_ref,
    probs_ref, hist_ref, fid_ref,
    gate_ref, send_amp, recv_amp, send_req, recv_req, send_wgt, recv_wgt,
    send_hst, recv_hst, send_ans, recv_ans, rank_hot, carry_ref, place_ref,
    send_sem, recv_sem,
):
    me = lax.axis_index("dev")
    barrier = pltpu.get_barrier_semaphore()

    def greet(k, c):
        pl.semaphore_signal(
            barrier, inc=1, device_id=(lax.rem(me + k, N),), device_id_type=MESH
        )
        return c

    lax.fori_loop(1, N, greet, 0)

    def exchange(which, src, dst, rows, pitch, src_block=None):
        def source(d):
            start = d * pitch if src_block is None else src_block(d)
            return src.at[pl.ds(start, rows), :]

        def send(k, c):
            d = lax.rem(me + k, N)
            pltpu.make_async_remote_copy(
                src_ref=source(d),
                dst_ref=dst.at[pl.ds(me * pitch, rows), :],
                send_sem=send_sem.at[which],
                recv_sem=recv_sem.at[which],
                device_id=(d,),
                device_id_type=MESH,
            ).start()
            return c

        lax.fori_loop(1, N, send, 0)
        pltpu.make_async_copy(
            source(me), dst.at[pl.ds(me * pitch, rows), :], recv_sem.at[which]
        ).start()

    def arrived(which, dst, rows):
        whole = dst.at[pl.ds(0, N * rows), :]
        pltpu.make_async_copy(whole, whole, recv_sem.at[which]).wait()

    def sent(which, dst, rows):
        most = dst.at[pl.ds(0, (N - 1) * rows), :]
        pltpu.make_async_copy(most, most, send_sem.at[which]).wait()

    entries = gate_entries(angles_ref[...])
    for kind in range(4):
        for part in range(2):
            gate_ref[2 * kind + part, pl.ds(0, 22), :] = entries[kind][part]

    def entry(kind, part, qubit, size):
        row = gate_ref[2 * kind + part, pl.ds(qubit, 1), :]
        row = jnp.broadcast_to(row, (8, 128))
        return row if size == 128 else jnp.concatenate([row] * (size // 128), axis=1)

    lane_re, lane_im = kron_matrix(entry, list(range(0, 7)), True)
    row_re, row_im = kron_matrix(entry, list(range(7, 15)), False)
    field = jnp.concatenate(
        [state_ref[pl.ds(0, 256, stride=2), :], state_ref[pl.ds(1, 256, stride=2), :]], axis=1
    )
    lane_gate = jnp.concatenate(
        [
            jnp.concatenate([lane_re, lane_im], axis=1),
            jnp.concatenate([-lane_im, lane_re], axis=1),
        ],
        axis=0,
    )
    field = dot3(field, lane_gate)
    product = dot3(jnp.concatenate([row_re, row_im], axis=0), field)
    amp_re = product[:256, :128] - product[256:, 128:]
    amp_im = product[:256, 128:] + product[256:, :128]
    for half in range(2):
        send_amp[pl.ds(half, 128, stride=4), :] = amp_re[half * 128 : (half + 1) * 128]
        send_amp[pl.ds(2 + half, 128, stride=4), :] = amp_im[half * 128 : (half + 1) * 128]
    pl.semaphore_wait(barrier, N - 1)
    exchange(0, send_amp, recv_amp, 4, 4)

    carry_ref[...] = jnp.zeros((128, 256), F32)
    place_ref[...] = jnp.zeros((256, 256), F32)
    before = jnp.where(iota((256, 256), 0) < iota((256, 256), 1), 1.0, 0.0).astype(BF16)
    prefix = jnp.concatenate([before, jnp.ones((256, 256), BF16)], axis=1)

    def route(step, c):
        lhs_parts, hot_parts = [], []
        carry = carry_ref[...]
        for sub in range(4):
            at = step * 8 + 2 * sub
            owner = jnp.concatenate(
                [high_ref[pl.ds(at, 1), :], high_ref[pl.ds(at + 1, 1), :]], axis=1
            )
            low = jnp.concatenate(
                [low_ref[pl.ds(at, 1), :], low_ref[pl.ds(at + 1, 1), :]], axis=1
            )
            mine = iota((128, 256), 0) == owner
            hot = jnp.where(mine, 1.0, 0.0).astype(BF16)
            counts = dot(hot, prefix)
            rank = jnp.sum(
                jnp.where(mine, counts[:, :256] + carry, 0.0), axis=0, keepdims=True
            ).astype(I32)
            carry = carry + counts[:, 256:]
            ranked = jnp.where(iota((256, 256), 0) == rank, 1.0, 0.0).astype(BF16)
            rank_hot[:, pl.ds(pl.multiple_of(step * 1024 + sub * 256, 256), 256)] = ranked
            hot_parts.append(ranked)
            low_part = (low & 255).astype(F32)
            high_part = ((low >> 8) + 1).astype(F32)
            lhs_parts.append(
                jnp.concatenate(
                    [jnp.where(mine, low_part, 0.0), jnp.where(mine, high_part, 0.0)], axis=0
                ).astype(BF16)
            )
        carry_ref[...] = carry
        place_ref[...] += lax.dot_general(
            jnp.concatenate(lhs_parts, axis=1),
            jnp.concatenate(hot_parts, axis=1),
            (((1,), (1,)), ((), ())),
            preferred_element_type=F32,
        )
        return c

    lax.fori_loop(0, 8, route, 0)
    asked = (place_ref[:128, :] + 256.0 * (place_ref[128:, :] - 1.0)).astype(I32)
    for half in range(2):
        send_req[pl.ds(half, 128, stride=2), :] = asked[:, half * 128 : (half + 1) * 128]
    exchange(1, send_req, recv_req, 2, 2)

    glob_re, glob_im = kron_matrix(entry, list(range(15, 22)), False)
    glob = jnp.concatenate(
        [
            jnp.concatenate([glob_re, -glob_im], axis=1),
            jnp.concatenate([glob_im, glob_re], axis=1),
        ],
        axis=0,
    )
    bins = iota((1, 1024), 1)
    local_code = jnp.zeros((256, 128), I32)
    global_code = jnp.zeros((128, 128), I32)
    row_id, g_id = iota((256, 128), 0), iota((128, 128), 0)
    local_mask = jnp.int32(0)
    other_mask = jnp.int32(0)
    other_code = jnp.int32(0)
    for k in range(10):
        qubit = marg_ref[k]
        in_lane, in_dev = qubit < 7, (qubit >= 7) & (qubit < 14)
        in_half, in_glob = qubit == 14, qubit >= 15
        place = jnp.where(in_half, 7, jnp.where(in_lane, qubit, 31))
        local_code += ((row_id >> place) & 1) << k
        local_mask += jnp.where(in_lane | in_half, 1 << k, 0)
        g_place = jnp.where(in_glob, qubit - 15, 31)
        global_code += ((g_id >> g_place) & 1) << k
        other_mask += jnp.where(in_glob | in_dev, 1 << k, 0)
        d_place = jnp.where(in_dev, qubit - 7, 31)
        other_code += ((me >> d_place) & 1) << k
    local_code = jnp.concatenate([local_code] * 8, axis=1)
    global_code = jnp.concatenate([global_code + other_code] * 8, axis=1)
    local_hot = jnp.where((bins & local_mask) == local_code, 1.0, 0.0).astype(BF16)
    global_hit = (bins & other_mask) == global_code

    arrived(0, recv_amp, 4)
    parts = [recv_amp[pl.ds(k, 128, stride=4), :] for k in range(4)]
    spread = jnp.concatenate(
        [
            jnp.concatenate([parts[0], parts[1]], axis=1),
            jnp.concatenate([parts[2], parts[3]], axis=1),
        ],
        axis=0,
    )
    final = dot3(glob, spread)
    weight = final[:128] * final[:128] + final[128:] * final[128:]
    for half in range(2):
        send_wgt[pl.ds(half, 128, stride=2), :] = weight[:, half * 128 : (half + 1) * 128]
    exchange(2, send_wgt, recv_wgt, 2, 2)

    folded = dot(jnp.concatenate(split(weight), axis=0), local_hot)
    folded = jnp.where(global_hit, folded[:128] + folded[128:], 0.0)
    partial = jnp.sum(folded, axis=0, keepdims=True)
    norm_part = jnp.sum(weight[:, :128] + weight[:, 128:], axis=0, keepdims=True)
    for row in range(8):
        send_hst[pl.ds(2 * row, 1), :] = partial[:, row * 128 : (row + 1) * 128]
        send_hst[pl.ds(2 * row + 1, 1), :] = norm_part
    exchange(3, send_hst, recv_hst, 2, 2, lambda d: (d // 16) * 2)

    arrived(1, recv_req, 2)
    arrived(2, recv_wgt, 2)
    table = jnp.concatenate(
        [recv_wgt[pl.ds(half, 128, stride=2), :].T for half in range(2)], axis=0
    )
    table = jnp.concatenate(split(table), axis=1)

    def answer(step, c):
        wanted = []
        for sub in range(16):
            wanted.append(recv_req[pl.ds(step * 16 + sub, 1), :])
        wanted = jnp.concatenate(wanted, axis=1)
        hot = jnp.where(iota((128, 2048), 0) == (wanted >> 7) & 127, 1.0, 0.0).astype(BF16)
        found = dot(table, jnp.concatenate([hot, hot], axis=0))
        found = select_rows(found, [bit_of(wanted, p) for p in (14, 6, 5, 4, 3)])
        found = pick_sublane(found, wanted & 7)
        for sub in range(16):
            at = (step * 8 + sub // 2) * 4 + sub % 2
            send_ans[pl.ds(at, 1), :] = found[:, sub * 128 : (sub + 1) * 128]
        return c

    lax.fori_loop(0, 16, answer, 0)
    fid_part = jnp.zeros((128, 128), F32)
    for half in range(2):
        valid = recv_req[pl.ds(half, 128, stride=2), :] >= 0
        fid_part += jnp.where(valid, send_ans[pl.ds(half, 128, stride=4), :], 0.0)
    fid_part = jnp.sum(fid_part, axis=0, keepdims=True)
    send_ans[pl.ds(2, 128, stride=4), :] = jnp.broadcast_to(fid_part, (128, 128))
    exchange(4, send_ans, recv_ans, 3, 4)

    arrived(3, recv_hst, 2)
    norm = jnp.sum(
        jnp.sum(recv_hst[pl.ds(1, 128, stride=2), :], axis=0, keepdims=True), axis=1, keepdims=True
    )
    bins_row = jnp.sum(recv_hst[pl.ds(0, 128, stride=2), :], axis=0, keepdims=True)
    bins_row = 1024.0 * (bins_row / norm)
    bins_row = pltpu.roll(bins_row, lax.rem(128 - lax.rem(me, 16) * 8, 128), 1)
    hist_ref[...] = bins_row[:, :8]

    arrived(4, recv_ans, 3)
    answers = jnp.concatenate(
        [recv_ans[pl.ds(half, 128, stride=4), :] for half in range(2)], axis=1
    )
    answers = jnp.concatenate(split(answers), axis=0)
    total = jnp.sum(
        jnp.sum(recv_ans[pl.ds(2, 128, stride=4), :], axis=0, keepdims=True), axis=1, keepdims=True
    )
    fid_ref[...] = 4194304.0 * (total / norm) / 1048576.0 - 1.0
    scale = 4194304.0 / norm

    def collect(step, c):
        owner = jnp.concatenate([high_ref[pl.ds(step * 8 + k, 1), :] for k in range(8)], axis=1)
        hot = rank_hot[:, pl.ds(pl.multiple_of(step * 1024, 1024), 1024)]
        found = dot(answers, hot)
        found = found[:128] + found[128:]
        found = select_rows(found, [bit_of(owner, p) for p in (6, 5, 4, 3)])
        found = pick_sublane(found, owner & 7) * scale
        for k in range(8):
            probs_ref[pl.ds(step * 8 + k, 1), :] = found[:, k * 128 : (k + 1) * 128]
        return c

    lax.fori_loop(0, 8, collect, 0)
    sent(0, send_amp, 4)
    sent(1, send_req, 2)
    sent(2, send_wgt, 2)
    sent(3, recv_hst, 2)
    sent(4, send_ans, 3)


def on_device(state, angles, sample_high, sample_low, marginal_qubits):
    vmem = pl.BlockSpec(memory_space=pltpu.VMEM)
    field = state.reshape(2, 256, 128).transpose(1, 0, 2).reshape(512, 128)
    probs, hist, fid = pl.pallas_call(
        kernel,
        out_shape=(
            jax.ShapeDtypeStruct((64, 128), F32),
            jax.ShapeDtypeStruct((1, 8), F32),
            jax.ShapeDtypeStruct((1, 1), F32),
        ),
        in_specs=[vmem, vmem, vmem, vmem, pl.BlockSpec(memory_space=pltpu.SMEM)],
        out_specs=(vmem, vmem, vmem),
        scratch_shapes=[
            pltpu.VMEM((8, 24, 128), F32),
            pltpu.VMEM((512, 128), F32),
            pltpu.VMEM((512, 128), F32),
            pltpu.VMEM((256, 128), I32),
            pltpu.VMEM((256, 128), I32),
            pltpu.VMEM((256, 128), F32),
            pltpu.VMEM((256, 128), F32),
            pltpu.VMEM((16, 128), F32),
            pltpu.VMEM((256, 128), F32),
            pltpu.VMEM((512, 128), F32),
            pltpu.VMEM((512, 128), F32),
            pltpu.VMEM((256, 8192), BF16),
            pltpu.VMEM((128, 256), F32),
            pltpu.VMEM((256, 256), F32),
            pltpu.SemaphoreType.DMA((5,)),
            pltpu.SemaphoreType.DMA((5,)),
        ],
        compiler_params=pltpu.CompilerParams(collective_id=0, has_side_effects=True),
    )(
        field,
        angles,
        sample_high.reshape(64, 128),
        sample_low.reshape(64, 128),
        marginal_qubits,
    )
    return probs.reshape(8192), hist.reshape(8), fid.reshape(())


def solution(mesh):
    return jax.shard_map(
        on_device,
        mesh=mesh,
        in_specs=(P(None, "dev"), P(), P("dev", None), P("dev"), P()),
        out_specs=(P("dev"), P("dev"), P()),
        check_vma=False,
    )
```

```python
import functools

import jax
import jax.numpy as jnp
from jax import lax
from jax.experimental import pallas as pl
from jax.experimental.pallas import tpu as pltpu
from jax.sharding import PartitionSpec as P

N = 128
MESH = pl.DeviceIdType.MESH
F32 = jnp.float32
BF16 = jnp.bfloat16
I32 = jnp.int32


def iota(shape, dim):
    return lax.broadcasted_iota(I32, shape, dim)


def dot(a, b):
    return jnp.dot(a, b, preferred_element_type=F32)


def split(x):
    high = x.astype(BF16)
    low = (x - high.astype(F32)).astype(BF16)
    return high, low


def dot3(a, b):
    a_high, a_low = split(a)
    b_high, b_low = split(b)
    return dot(a_high, b_high) + (dot(a_high, b_low) + dot(a_low, b_high))


def complex_mul(a, b):
    return (a[0] * b[0] - a[1] * b[1], a[0] * b[1] + a[1] * b[0])


def gate_entries(angles, trig_ref):
    count = angles.shape[1]
    packed = jnp.concatenate([angles, angles[1:2] + angles[2:3]], axis=0)
    trig_ref[...] = jnp.zeros((8, 128), F32)
    trig_ref[pl.ds(0, 4), pl.ds(0, count)] = jnp.sin(packed)
    trig_ref[pl.ds(4, 4), pl.ds(0, count)] = jnp.cos(packed)
    turned = trig_ref[...].T

    def column(k):
        return jnp.broadcast_to(turned[:24, k : k + 1], (24, 128))

    sin_t, sin_f, sin_l, sin_fl, cos_t, cos_f, cos_l, cos_fl = (column(k) for k in range(8))
    return [
        (cos_t, jnp.zeros_like(cos_t)),
        (-cos_l * sin_t, -sin_l * sin_t),
        (cos_f * sin_t, sin_f * sin_t),
        (cos_fl * cos_t, sin_fl * cos_t),
    ]


def kron_matrix(entry, qubits, transposed):
    size = 2 ** len(qubits)
    lane, sub = iota((8, size), 1), iota((8, size), 0)

    def factor_rows(place, qubit):
        bit = (lane >> place) & 1 == 1

        def choose(zero, one):
            return tuple(
                jnp.where(bit, entry(one, part, qubit, size), entry(zero, part, qubit, size))
                for part in range(2)
            )

        if transposed:
            return choose(0, 2), choose(1, 3)
        return choose(0, 1), choose(2, 3)

    mat = None
    for place, qubit in enumerate(qubits):
        row_zero, row_one = factor_rows(place, qubit)
        if place < 3:
            bit = (sub >> place) & 1 == 1
            factor = tuple(jnp.where(bit, row_one[k], row_zero[k]) for k in range(2))
            mat = factor if mat is None else complex_mul(mat, factor)
        else:
            count = mat[0].shape[0] // 8
            halves = []
            for row in (row_zero, row_one):
                wide = tuple(jnp.concatenate([x] * count, axis=0) for x in row)
                halves.append(complex_mul(mat, wide))
            mat = tuple(jnp.concatenate([halves[0][k], halves[1][k]], axis=0) for k in range(2))
    return mat


def select_rows(values, bits):
    for bit in bits:
        half = values.shape[0] // 2
        values = jnp.where(bit, values[half:], values[:half])
    return values


def pick_sublane(values, index):
    hit = iota(values.shape, 0) == index
    return jnp.sum(jnp.where(hit, values, 0.0), axis=0, keepdims=True)


def bit_of(x, place):
    return (x >> place) & 1 == 1


def kernel(
    state_hbm, angles_hbm, high_hbm, low_hbm, marg_hbm,
    probs_ref, hist_ref, fid_ref,
    state_ref, angles_ref, high_ref, low_ref, marg_ref, trig_ref, gate_ref, send_amp, recv_amp, send_req, recv_req, send_wgt, recv_wgt,
    send_hst, recv_hst, send_ans, recv_ans, send_fid, recv_fid,
    rank_hot, rank_ref, seen_ref, place_ref, want_hot,
    send_sem, recv_sem, load_sem,
):
    me = lax.axis_index("dev")
    loads = [
        pltpu.make_async_copy(src, dst, load_sem.at[k])
        for k, (src, dst) in enumerate(
            [
                (angles_hbm, angles_ref),
                (state_hbm, state_ref),
                (high_hbm, high_ref),
                (low_hbm, low_ref),
                (marg_hbm, marg_ref),
            ]
        )
    ]
    for load in loads:
        load.start()
    barrier = pltpu.get_barrier_semaphore()

    def greet(k, c):
        pl.semaphore_signal(
            barrier, inc=1, device_id=(lax.rem(me + k, N),), device_id_type=MESH
        )
        return c

    lax.fori_loop(1, N, greet, 0, unroll=8)

    def exchange(which, src, dst, rows, pitch, src_block=None):
        def source(d):
            start = d * pitch if src_block is None else src_block(d)
            return src.at[pl.ds(start, rows), :]

        def send(k, c):
            d = lax.rem(me + k, N)
            pltpu.make_async_remote_copy(
                src_ref=source(d),
                dst_ref=dst.at[pl.ds(me * pitch, rows), :],
                send_sem=send_sem.at[which],
                recv_sem=recv_sem.at[which],
                device_id=(d,),
                device_id_type=MESH,
            ).start()
            return c

        lax.fori_loop(1, N, send, 0, unroll=4)
        pltpu.make_async_copy(
            source(me), dst.at[pl.ds(me * pitch, rows), :], recv_sem.at[which]
        ).start()

    def arrived(which, dst, rows):
        whole = dst.at[pl.ds(0, N * rows), :]
        pltpu.make_async_copy(whole, whole, recv_sem.at[which]).wait()

    def sent(which, dst, rows):
        most = dst.at[pl.ds(0, (N - 1) * rows), :]
        pltpu.make_async_copy(most, most, send_sem.at[which]).wait()

    loads[0].wait()
    entries = gate_entries(angles_ref[...], trig_ref)
    for kind in range(4):
        for part in range(2):
            gate_ref[2 * kind + part, :, :] = entries[kind][part]

    def entry(kind, part, qubit, size):
        row = gate_ref[2 * kind + part, pl.ds(qubit, 1), :]
        row = jnp.broadcast_to(row, (8, 128))
        return row if size == 128 else jnp.concatenate([row] * (size // 128), axis=1)

    lane_re, lane_im = kron_matrix(entry, list(range(0, 7)), True)
    row_re, row_im = kron_matrix(entry, list(range(7, 15)), False)
    for load in loads[1:]:
        load.wait()
    field = jnp.concatenate(
        [state_ref[pl.ds(0, 256, stride=2), :], state_ref[pl.ds(1, 256, stride=2), :]], axis=1
    )
    lane_gate = jnp.concatenate(
        [
            jnp.concatenate([lane_re, lane_im], axis=1),
            jnp.concatenate([-lane_im, lane_re], axis=1),
        ],
        axis=0,
    )
    field = dot3(field, lane_gate)
    product = dot3(jnp.concatenate([row_re, row_im], axis=0), field)
    amp_re = product[:256, :128] - product[256:, 128:]
    amp_im = product[:256, 128:] + product[256:, :128]
    for half in range(2):
        send_amp[pl.ds(half, 128, stride=4), :] = amp_re[half * 128 : (half + 1) * 128]
        send_amp[pl.ds(2 + half, 128, stride=4), :] = amp_im[half * 128 : (half + 1) * 128]

    ahead = jnp.where(iota((512, 256), 0) < iota((512, 256), 1), 1.0, 0.0)
    ahead = jnp.where(iota((512, 256), 0) >= 256, 1.0, ahead).astype(BF16)
    seen_ref[...] = jnp.zeros((128, 256), BF16)

    def owners(step, sub):
        at = step * 8 + 2 * sub
        row = jnp.concatenate(
            [high_ref[pl.ds(at, 1), :], high_ref[pl.ds(at + 1, 1), :]], axis=1
        )
        return iota((128, 256), 0) == row

    def rank(step, c):
        seen = seen_ref[...]
        rows, hits = [], []
        for sub in range(4):
            mine = owners(step, sub)
            hot = jnp.where(mine, 1.0, 0.0).astype(BF16)
            rows.append(jnp.concatenate([hot, seen], axis=1))
            hits.append(mine)
            seen = seen + hot
        seen_ref[...] = seen
        counts = dot(jnp.concatenate(rows, axis=0), ahead)
        for sub in range(4):
            ranks = jnp.sum(
                jnp.where(hits[sub], counts[128 * sub : 128 * (sub + 1)], 0.0),
                axis=0,
                keepdims=True,
            )
            for half in range(2):
                rank_ref[pl.ds(step * 8 + 2 * sub + half, 1), :] = ranks[
                    :, half * 128 : (half + 1) * 128
                ].astype(I32)
        return c

    lax.fori_loop(0, 8, rank, 0)
    pl.semaphore_wait(barrier, N - 1)
    exchange(0, send_amp, recv_amp, 4, 4)

    place_ref[...] = jnp.zeros((256, 256), F32)

    def route(step, c):
        lhs_parts, hot_parts = [], []
        for sub in range(4):
            at = step * 8 + 2 * sub
            low = jnp.concatenate(
                [low_ref[pl.ds(at, 1), :], low_ref[pl.ds(at + 1, 1), :]], axis=1
            )
            ranks = jnp.concatenate(
                [rank_ref[pl.ds(at, 1), :], rank_ref[pl.ds(at + 1, 1), :]], axis=1
            )
            mine = owners(step, sub)
            ranked = jnp.where(iota((256, 256), 0) == ranks, 1.0, 0.0).astype(BF16)
            rank_hot[:, pl.ds(pl.multiple_of(step * 1024 + sub * 256, 256), 256)] = ranked
            hot_parts.append(ranked)
            low_part = (low & 255).astype(F32)
            high_part = ((low >> 8) + 1).astype(F32)
            lhs_parts.append(
                jnp.concatenate(
                    [jnp.where(mine, low_part, 0.0), jnp.where(mine, high_part, 0.0)], axis=0
                ).astype(BF16)
            )
        place_ref[...] += lax.dot_general(
            jnp.concatenate(lhs_parts, axis=1),
            jnp.concatenate(hot_parts, axis=1),
            (((1,), (1,)), ((), ())),
            preferred_element_type=F32,
        )
        return c

    lax.fori_loop(0, 8, route, 0)
    asked = (place_ref[:128, :] + 256.0 * (place_ref[128:, :] - 1.0)).astype(I32)
    for half in range(2):
        send_req[pl.ds(half, 128, stride=2), :] = asked[:, half * 128 : (half + 1) * 128]
    exchange(1, send_req, recv_req, 2, 2)

    glob_re, glob_im = kron_matrix(entry, list(range(15, 22)), False)
    glob = jnp.concatenate(
        [
            jnp.concatenate([glob_re, -glob_im], axis=1),
            jnp.concatenate([glob_im, glob_re], axis=1),
        ],
        axis=0,
    )
    bins = iota((1, 1024), 1)
    local_code = jnp.zeros((256, 128), I32)
    global_code = jnp.zeros((128, 128), I32)
    row_id, g_id = iota((256, 128), 0), iota((128, 128), 0)
    local_mask = jnp.int32(0)
    other_mask = jnp.int32(0)
    other_code = jnp.int32(0)
    for k in range(10):
        qubit = marg_ref[k]
        in_lane, in_dev = qubit < 7, (qubit >= 7) & (qubit < 14)
        in_half, in_glob = qubit == 14, qubit >= 15
        place = jnp.where(in_half, 7, jnp.where(in_lane, qubit, 31))
        local_code += ((row_id >> place) & 1) << k
        local_mask += jnp.where(in_lane | in_half, 1 << k, 0)
        g_place = jnp.where(in_glob, qubit - 15, 31)
        global_code += ((g_id >> g_place) & 1) << k
        other_mask += jnp.where(in_glob | in_dev, 1 << k, 0)
        d_place = jnp.where(in_dev, qubit - 7, 31)
        other_code += ((me >> d_place) & 1) << k
    local_code = jnp.concatenate([local_code] * 8, axis=1)
    global_code = jnp.concatenate([global_code + other_code] * 8, axis=1)
    local_hot = jnp.where((bins & local_mask) == local_code, 1.0, 0.0).astype(BF16)
    global_hit = (bins & other_mask) == global_code

    arrived(0, recv_amp, 4)
    parts = [recv_amp[pl.ds(k, 128, stride=4), :] for k in range(4)]
    spread = jnp.concatenate(
        [
            jnp.concatenate([parts[0], parts[1]], axis=1),
            jnp.concatenate([parts[2], parts[3]], axis=1),
        ],
        axis=0,
    )
    final = dot3(glob, spread)
    weight = final[:128] * final[:128] + final[128:] * final[128:]
    for half in range(2):
        send_wgt[pl.ds(half, 128, stride=2), :] = weight[:, half * 128 : (half + 1) * 128]
    exchange(2, send_wgt, recv_wgt, 2, 2)

    folded = dot(jnp.concatenate(split(weight), axis=0), local_hot)
    folded = jnp.where(global_hit, folded[:128] + folded[128:], 0.0)
    partial = jnp.sum(folded, axis=0, keepdims=True)
    norm_part = jnp.sum(weight[:, :128] + weight[:, 128:], axis=0, keepdims=True)
    for row in range(8):
        send_hst[pl.ds(2 * row, 1), :] = partial[:, row * 128 : (row + 1) * 128]
        send_hst[pl.ds(2 * row + 1, 1), :] = norm_part
    exchange(3, send_hst, recv_hst, 2, 2, lambda d: (d // 16) * 2)

    my_z, my_x, my_yc = me // 32, lax.rem(me // 8, 4), lax.rem(me, 8)

    def far(j):
        return 2 + 3 * j + 3 * (j // 2) + 2 * (j // 3)

    def chunk_base(k):
        z = lax.rem(my_z + far(k // 4), 4)
        x = lax.rem(my_x + far(lax.rem(k, 4)), 4)
        return z * 32 + x * 8

    def wanted_of(k):
        at = chunk_base(k) * 2
        return jnp.concatenate([recv_req[pl.ds(at + r, 1), :] for r in range(16)], axis=1)

    arrived(1, recv_req, 2)

    def prepare(k, c):
        column = (wanted_of(k) >> 7) & 127
        want_hot[:, pl.ds(pl.multiple_of(k * 2048, 2048), 2048)] = jnp.where(
            iota((128, 2048), 0) == column, 1.0, 0.0
        ).astype(BF16)
        return c

    lax.fori_loop(0, 16, prepare, 0)

    arrived(2, recv_wgt, 2)
    table = jnp.concatenate(
        [recv_wgt[pl.ds(half, 128, stride=2), :].T for half in range(2)], axis=0
    )
    table = jnp.concatenate(split(table), axis=1)

    def answer(k):
        hot = want_hot[:, pl.ds(pl.multiple_of(k * 2048, 2048), 2048)]
        found = dot(table, jnp.concatenate([hot, hot], axis=0))
        wanted = wanted_of(k)
        found = select_rows(found, [bit_of(wanted, p) for p in (14, 6, 5, 4, 3)])
        found = pick_sublane(found, wanted & 7)
        at = chunk_base(k) * 2
        for r in range(16):
            send_ans[pl.ds(at + r, 1), :] = found[:, r * 128 : (r + 1) * 128]

    def reply(d):
        pltpu.make_async_remote_copy(
            src_ref=send_ans.at[pl.ds(d * 2, 2), :],
            dst_ref=recv_ans.at[pl.ds(me * 2, 2), :],
            send_sem=send_sem.at[4],
            recv_sem=recv_sem.at[4],
            device_id=(d,),
            device_id_type=MESH,
        ).start()

    def reply_chunk(k):
        base = chunk_base(k)
        for j in range(8):
            reply(base + j)

    def two_chunks(step, c):
        answer(2 * step)
        answer(2 * step + 1)
        reply_chunk(2 * step)
        reply_chunk(2 * step + 1)
        return c

    lax.fori_loop(0, 7, two_chunks, 0)
    answer(14)
    answer(15)
    reply_chunk(14)
    for j in range(1, 8):
        reply(me - my_yc + lax.rem(my_yc + j, 8))
    pltpu.make_async_copy(
        send_ans.at[pl.ds(me * 2, 2), :], recv_ans.at[pl.ds(me * 2, 2), :], recv_sem.at[4]
    ).start()
    fid_part = jnp.sum(
        jnp.where(recv_req[...] >= 0, send_ans[...], 0.0), axis=0, keepdims=True
    )
    send_fid[...] = jnp.broadcast_to(fid_part, (8, 128))
    exchange(5, send_fid, recv_fid, 1, 1, lambda d: 0)

    arrived(3, recv_hst, 2)
    norm = jnp.sum(
        jnp.sum(recv_hst[pl.ds(1, 128, stride=2), :], axis=0, keepdims=True), axis=1, keepdims=True
    )
    bins_row = jnp.sum(recv_hst[pl.ds(0, 128, stride=2), :], axis=0, keepdims=True)
    bins_row = 1024.0 * (bins_row / norm)
    bins_row = pltpu.roll(bins_row, lax.rem(128 - lax.rem(me, 16) * 8, 128), 1)
    hist_ref[...] = bins_row[:, :8]

    scale = 4194304.0 / norm
    arrived(4, recv_ans, 2)
    answers = jnp.concatenate(
        [recv_ans[pl.ds(half, 128, stride=2), :] for half in range(2)], axis=1
    )
    answers = jnp.concatenate(split(answers), axis=0)

    def collect(step, c):
        owner = jnp.concatenate([high_ref[pl.ds(step * 8 + k, 1), :] for k in range(8)], axis=1)
        hot = rank_hot[:, pl.ds(pl.multiple_of(step * 1024, 1024), 1024)]
        found = dot(answers, hot)
        found = found[:128] + found[128:]
        found = select_rows(found, [bit_of(owner, p) for p in (6, 5, 4, 3)])
        found = pick_sublane(found, owner & 7) * scale
        for k in range(8):
            probs_ref[pl.ds(step * 8 + k, 1), :] = found[:, k * 128 : (k + 1) * 128]
        return c

    lax.fori_loop(0, 8, collect, 0)

    arrived(5, recv_fid, 1)
    total = jnp.sum(
        jnp.sum(recv_fid[...], axis=0, keepdims=True), axis=1, keepdims=True
    )
    fid_ref[...] = 4194304.0 * (total / norm) / 1048576.0 - 1.0
    sent(0, send_amp, 4)
    sent(1, send_req, 2)
    sent(2, send_wgt, 2)
    sent(3, recv_hst, 2)
    sent(4, send_ans, 2)
    sent(5, recv_fid, 1)


def on_device(state, angles, sample_high, sample_low, marginal_qubits):
    vmem = pl.BlockSpec(memory_space=pltpu.VMEM)
    field = state.reshape(2, 256, 128).transpose(1, 0, 2).reshape(512, 128)
    probs, hist, fid = pl.pallas_call(
        kernel,
        out_shape=(
            jax.ShapeDtypeStruct((64, 128), F32),
            jax.ShapeDtypeStruct((1, 8), F32),
            jax.ShapeDtypeStruct((1, 1), F32),
        ),
        in_specs=[pl.BlockSpec(memory_space=pl.ANY)] * 5,
        out_specs=(vmem, vmem, vmem),
        scratch_shapes=[
            pltpu.VMEM((512, 128), F32),
            pltpu.VMEM((3, 22), F32),
            pltpu.VMEM((64, 128), I32),
            pltpu.VMEM((64, 128), I32),
            pltpu.SMEM((10,), I32),
            pltpu.VMEM((8, 128), F32),
            pltpu.VMEM((8, 24, 128), F32),
            pltpu.VMEM((512, 128), F32),
            pltpu.VMEM((512, 128), F32),
            pltpu.VMEM((256, 128), I32),
            pltpu.VMEM((256, 128), I32),
            pltpu.VMEM((256, 128), F32),
            pltpu.VMEM((256, 128), F32),
            pltpu.VMEM((16, 128), F32),
            pltpu.VMEM((256, 128), F32),
            pltpu.VMEM((256, 128), F32),
            pltpu.VMEM((256, 128), F32),
            pltpu.VMEM((8, 128), F32),
            pltpu.VMEM((128, 128), F32),
            pltpu.VMEM((256, 8192), BF16),
            pltpu.VMEM((64, 128), I32),
            pltpu.VMEM((128, 256), BF16),
            pltpu.VMEM((256, 256), F32),
            pltpu.VMEM((128, 32768), BF16),
            pltpu.SemaphoreType.DMA((6,)),
            pltpu.SemaphoreType.DMA((6,)),
            pltpu.SemaphoreType.DMA((5,)),
        ],
        compiler_params=pltpu.CompilerParams(collective_id=0, has_side_effects=True),
    )(
        field,
        angles.T,
        sample_high.reshape(64, 128),
        sample_low.reshape(64, 128),
        marginal_qubits,
    )
    return probs.reshape(8192), hist.reshape(8), fid.reshape(())


def solution(mesh):
    return jax.shard_map(
        on_device,
        mesh=mesh,
        in_specs=(P(None, "dev"), P(), P("dev", None), P("dev"), P()),
        out_specs=(P("dev"), P("dev"), P()),
        check_vma=False,
    )
```

```python
import functools

import jax
import jax.numpy as jnp
from jax import lax
from jax.experimental import pallas as pl
from jax.experimental.pallas import tpu as pltpu
from jax.sharding import PartitionSpec as P

N = 128
MESH = pl.DeviceIdType.MESH
F32 = jnp.float32
BF16 = jnp.bfloat16
I32 = jnp.int32


def iota(shape, dim):
    return lax.broadcasted_iota(I32, shape, dim)


def dot(a, b):
    return jnp.dot(a, b, preferred_element_type=F32)


def split(x):
    high = x.astype(BF16)
    low = (x - high.astype(F32)).astype(BF16)
    return high, low


def dot3(a, b):
    a_high, a_low = split(a)
    b_high, b_low = split(b)
    return dot(a_high, b_high) + (dot(a_high, b_low) + dot(a_low, b_high))


def complex_mul(a, b):
    return (a[0] * b[0] - a[1] * b[1], a[0] * b[1] + a[1] * b[0])


def gate_entries(angles, trig_ref):
    count = angles.shape[1]
    packed = jnp.concatenate([angles, angles[1:2] + angles[2:3]], axis=0)
    trig_ref[...] = jnp.zeros((8, 128), F32)
    trig_ref[pl.ds(0, 4), pl.ds(0, count)] = jnp.sin(packed)
    trig_ref[pl.ds(4, 4), pl.ds(0, count)] = jnp.cos(packed)
    turned = trig_ref[...].T

    def column(k):
        return jnp.broadcast_to(turned[:24, k : k + 1], (24, 128))

    sin_t, sin_f, sin_l, sin_fl, cos_t, cos_f, cos_l, cos_fl = (column(k) for k in range(8))
    return [
        (cos_t, jnp.zeros_like(cos_t)),
        (-cos_l * sin_t, -sin_l * sin_t),
        (cos_f * sin_t, sin_f * sin_t),
        (cos_fl * cos_t, sin_fl * cos_t),
    ]


def kron_matrix(entry, qubits, transposed):
    size = 2 ** len(qubits)
    lane, sub = iota((8, size), 1), iota((8, size), 0)

    def factor_rows(place, qubit):
        bit = (lane >> place) & 1 == 1

        def choose(zero, one):
            return tuple(
                jnp.where(bit, entry(one, part, qubit, size), entry(zero, part, qubit, size))
                for part in range(2)
            )

        if transposed:
            return choose(0, 2), choose(1, 3)
        return choose(0, 1), choose(2, 3)

    mat = None
    for place, qubit in enumerate(qubits):
        row_zero, row_one = factor_rows(place, qubit)
        if place < 3:
            bit = (sub >> place) & 1 == 1
            factor = tuple(jnp.where(bit, row_one[k], row_zero[k]) for k in range(2))
            mat = factor if mat is None else complex_mul(mat, factor)
        else:
            count = mat[0].shape[0] // 8
            halves = []
            for row in (row_zero, row_one):
                wide = tuple(jnp.concatenate([x] * count, axis=0) for x in row)
                halves.append(complex_mul(mat, wide))
            mat = tuple(jnp.concatenate([halves[0][k], halves[1][k]], axis=0) for k in range(2))
    return mat


def select_rows(values, bits):
    for bit in bits:
        half = values.shape[0] // 2
        values = jnp.where(bit, values[half:], values[:half])
    return values


def pick_sublane(values, index):
    hit = iota(values.shape, 0) == index
    return jnp.sum(jnp.where(hit, values, 0.0), axis=0, keepdims=True)


def one_hot(ids, rows):
    one, zero = jnp.ones(ids.shape, BF16), jnp.zeros(ids.shape, BF16)
    return jnp.concatenate([jnp.where(ids == row, one, zero) for row in rows], axis=1)


def bit_of(x, place):
    return (x >> place) & 1 == 1


def kernel(
    state_hbm, angles_hbm, high_hbm, low_hbm, marg_hbm,
    probs_ref, hist_ref, fid_ref,
    state_ref, angles_ref, high_ref, low_ref, marg_ref, trig_ref, gate_ref, send_amp, recv_amp, send_req, recv_req, send_wgt, recv_wgt,
    send_hst, recv_hst, send_ans, recv_ans, send_fid, recv_fid,
    rank_hot, rank_ref, seen_ref, place_ref, want_hot, ids_ref,
    send_sem, recv_sem, load_sem,
):
    me = lax.axis_index("dev")
    loads = [
        pltpu.make_async_copy(src, dst, load_sem.at[k])
        for k, (src, dst) in enumerate(
            [
                (angles_hbm, angles_ref),
                (state_hbm, state_ref),
                (high_hbm, high_ref),
                (low_hbm, low_ref),
                (marg_hbm, marg_ref),
            ]
        )
    ]
    my_z, my_x = me // 32, lax.rem(me // 8, 4)
    my_y, my_core = lax.rem(me // 2, 4), lax.rem(me, 2)

    def far(j):
        return 2 + 3 * j + 3 * (j // 2) + 2 * (j // 3)

    def chunk_base(k):
        z = lax.rem(my_z + far(k // 4), 4)
        x = lax.rem(my_x + far(lax.rem(k, 4)), 4)
        return z * 32 + x * 8

    inner = [lax.rem(my_y + far(j // 2), 4) * 2 + lax.rem(my_core + 1 + j, 2) for j in range(8)]

    def others(act):
        def chunk(k, c):
            base = chunk_base(k)
            for j in range(8):
                act(base + inner[j])
            return c

        lax.fori_loop(0, 15, chunk, 0)
        base = my_z * 32 + my_x * 8
        for j in range(7):
            act(base + inner[j])

    barrier = pltpu.get_barrier_semaphore()

    others(
        lambda d: pl.semaphore_signal(barrier, inc=1, device_id=(d,), device_id_type=MESH)
    )
    for load in loads:
        load.start()

    def exchange(which, src, dst, rows, pitch, src_block=None):
        def source(d):
            start = d * pitch if src_block is None else src_block(d)
            return src.at[pl.ds(start, rows), :]

        def send(d):
            pltpu.make_async_remote_copy(
                src_ref=source(d),
                dst_ref=dst.at[pl.ds(me * pitch, rows), :],
                send_sem=send_sem.at[which],
                recv_sem=recv_sem.at[which],
                device_id=(d,),
                device_id_type=MESH,
            ).start()

        others(send)
        pltpu.make_async_copy(
            source(me), dst.at[pl.ds(me * pitch, rows), :], recv_sem.at[which]
        ).start()

    def arrived(which, dst, rows):
        whole = dst.at[pl.ds(0, N * rows), :]
        pltpu.make_async_copy(whole, whole, recv_sem.at[which]).wait()

    def sent(which, dst, rows):
        most = dst.at[pl.ds(0, (N - 1) * rows), :]
        pltpu.make_async_copy(most, most, send_sem.at[which]).wait()

    ids_ref[...] = iota((256, 128), 0).astype(F32).astype(BF16)
    loads[0].wait()
    entries = gate_entries(angles_ref[...], trig_ref)
    for kind in range(4):
        for part in range(2):
            gate_ref[2 * kind + part, :, :] = entries[kind][part]

    def entry(kind, part, qubit, size):
        row = gate_ref[2 * kind + part, pl.ds(qubit, 1), :]
        row = jnp.broadcast_to(row, (8, 128))
        return row if size == 128 else jnp.concatenate([row] * (size // 128), axis=1)

    lane_re, lane_im = kron_matrix(entry, list(range(0, 7)), True)
    row_re, row_im = kron_matrix(entry, list(range(7, 15)), False)
    for load in loads[1:]:
        load.wait()
    field = jnp.concatenate(
        [state_ref[pl.ds(0, 256, stride=2), :], state_ref[pl.ds(1, 256, stride=2), :]], axis=1
    )
    lane_gate = jnp.concatenate(
        [
            jnp.concatenate([lane_re, lane_im], axis=1),
            jnp.concatenate([-lane_im, lane_re], axis=1),
        ],
        axis=0,
    )
    field = dot3(field, lane_gate)
    product = dot3(jnp.concatenate([row_re, row_im], axis=0), field)
    amp_re = product[:256, :128] - product[256:, 128:]
    amp_im = product[:256, 128:] + product[256:, :128]
    for half in range(2):
        send_amp[pl.ds(half, 128, stride=4), :] = amp_re[half * 128 : (half + 1) * 128]
        send_amp[pl.ds(2 + half, 128, stride=4), :] = amp_im[half * 128 : (half + 1) * 128]

    ahead = jnp.where(iota((512, 256), 0) < iota((512, 256), 1), 1.0, 0.0)
    ahead = jnp.where(iota((512, 256), 0) >= 256, 1.0, ahead).astype(BF16)
    seen_ref[...] = jnp.zeros((128, 256), BF16)

    def rank(step, c):
        seen = seen_ref[...]
        rows, hits = [], []
        for sub in range(4):
            at = step * 8 + 2 * sub
            owner = [high_ref[pl.ds(at + half, 1), :] for half in range(2)]
            hot = one_hot(ids_ref[pl.ds(0, 128), :], [x.astype(F32).astype(BF16) for x in owner])
            mine = iota((128, 256), 0) == jnp.concatenate(owner, axis=1)
            rows.append(jnp.concatenate([hot, seen], axis=1))
            hits.append(mine)
            seen = seen + hot
        seen_ref[...] = seen
        counts = dot(jnp.concatenate(rows, axis=0), ahead)
        for sub in range(4):
            ranks = jnp.sum(
                jnp.where(hits[sub], counts[128 * sub : 128 * (sub + 1)], 0.0),
                axis=0,
                keepdims=True,
            )
            for half in range(2):
                rank_ref[pl.ds(step * 8 + 2 * sub + half, 1), :] = ranks[
                    :, half * 128 : (half + 1) * 128
                ]
        return c

    lax.fori_loop(0, 8, rank, 0, unroll=4)
    pl.semaphore_wait(barrier, N - 1)
    exchange(0, send_amp, recv_amp, 4, 4)

    place_ref[...] = jnp.zeros((256, 256), F32)

    def route(step, c):
        lhs_parts, hot_parts = [], []
        ids = ids_ref[...]
        none = jnp.zeros((128, 128), BF16)
        for sub in range(8):
            at = step * 8 + sub
            low = low_ref[pl.ds(at, 1), :]
            low_part = (low & 255).astype(F32).astype(BF16)
            high_part = ((low >> 8) + 1).astype(F32).astype(BF16)
            mine = ids[:128] == high_ref[pl.ds(at, 1), :].astype(F32).astype(BF16)
            ranked = one_hot(ids, [rank_ref[pl.ds(at, 1), :].astype(BF16)])
            rank_hot[:, pl.ds(pl.multiple_of(step * 1024 + sub * 128, 128), 128)] = ranked
            hot_parts.append(ranked)
            lhs_parts.append(
                jnp.concatenate(
                    [jnp.where(mine, low_part, none), jnp.where(mine, high_part, none)], axis=0
                )
            )
        place_ref[...] += lax.dot_general(
            jnp.concatenate(lhs_parts, axis=1),
            jnp.concatenate(hot_parts, axis=1),
            (((1,), (1,)), ((), ())),
            preferred_element_type=F32,
        )
        return c

    lax.fori_loop(0, 8, route, 0, unroll=2)
    asked = (place_ref[:128, :] + 256.0 * (place_ref[128:, :] - 1.0)).astype(I32)
    for half in range(2):
        send_req[pl.ds(half, 128, stride=2), :] = asked[:, half * 128 : (half + 1) * 128]
    exchange(1, send_req, recv_req, 2, 2)

    glob_re, glob_im = kron_matrix(entry, list(range(15, 22)), False)
    glob = jnp.concatenate(
        [
            jnp.concatenate([glob_re, -glob_im], axis=1),
            jnp.concatenate([glob_im, glob_re], axis=1),
        ],
        axis=0,
    )
    bins = iota((1, 1024), 1)
    local_code = jnp.zeros((256, 128), I32)
    global_code = jnp.zeros((128, 128), I32)
    row_id, g_id = iota((256, 128), 0), iota((128, 128), 0)
    local_mask = jnp.int32(0)
    other_mask = jnp.int32(0)
    other_code = jnp.int32(0)
    for k in range(10):
        qubit = marg_ref[k]
        in_lane, in_dev = qubit < 7, (qubit >= 7) & (qubit < 14)
        in_half, in_glob = qubit == 14, qubit >= 15
        place = jnp.where(in_half, 7, jnp.where(in_lane, qubit, 31))
        local_code += ((row_id >> place) & 1) << k
        local_mask += jnp.where(in_lane | in_half, 1 << k, 0)
        g_place = jnp.where(in_glob, qubit - 15, 31)
        global_code += ((g_id >> g_place) & 1) << k
        other_mask += jnp.where(in_glob | in_dev, 1 << k, 0)
        d_place = jnp.where(in_dev, qubit - 7, 31)
        other_code += ((me >> d_place) & 1) << k
    local_code = jnp.concatenate([local_code] * 8, axis=1)
    global_code = jnp.concatenate([global_code + other_code] * 8, axis=1)
    local_hot = jnp.where((bins & local_mask) == local_code, 1.0, 0.0).astype(BF16)
    global_hit = (bins & other_mask) == global_code

    arrived(0, recv_amp, 4)
    parts = [recv_amp[pl.ds(k, 128, stride=4), :] for k in range(4)]
    spread = jnp.concatenate(
        [
            jnp.concatenate([parts[0], parts[1]], axis=1),
            jnp.concatenate([parts[2], parts[3]], axis=1),
        ],
        axis=0,
    )
    final = dot3(glob, spread)
    weight = final[:128] * final[:128] + final[128:] * final[128:]
    for half in range(2):
        send_wgt[pl.ds(half, 128, stride=2), :] = weight[:, half * 128 : (half + 1) * 128]
    exchange(2, send_wgt, recv_wgt, 2, 2)

    folded = dot(jnp.concatenate(split(weight), axis=0), local_hot)
    folded = jnp.where(global_hit, folded[:128] + folded[128:], 0.0)
    partial = jnp.sum(folded, axis=0, keepdims=True)
    norm_part = jnp.sum(weight[:, :128] + weight[:, 128:], axis=0, keepdims=True)
    for row in range(8):
        send_hst[pl.ds(2 * row, 1), :] = partial[:, row * 128 : (row + 1) * 128]
        send_hst[pl.ds(2 * row + 1, 1), :] = norm_part
    exchange(3, send_hst, recv_hst, 2, 2, lambda d: (d // 16) * 2)

    def wanted_of(k):
        at = chunk_base(k) * 2
        return jnp.concatenate([recv_req[pl.ds(at + r, 1), :] for r in range(16)], axis=1)

    arrived(1, recv_req, 2)

    def prepare(k, c):
        at = chunk_base(k) * 2
        rows = [
            ((recv_req[pl.ds(at + r, 1), :] >> 7) & 127).astype(F32).astype(BF16)
            for r in range(16)
        ]
        want_hot[:, pl.ds(pl.multiple_of(k * 2048, 2048), 2048)] = one_hot(
            ids_ref[pl.ds(0, 128), :], rows
        )
        return c

    lax.fori_loop(0, 16, prepare, 0)

    arrived(2, recv_wgt, 2)
    table = jnp.concatenate(
        [recv_wgt[pl.ds(half, 128, stride=2), :].T for half in range(2)], axis=0
    )
    table = jnp.concatenate(split(table), axis=1)

    def answer(k):
        hot = want_hot[:, pl.ds(pl.multiple_of(k * 2048, 2048), 2048)]
        found = dot(table, jnp.concatenate([hot, hot], axis=0))
        wanted = wanted_of(k)
        found = select_rows(found, [bit_of(wanted, p) for p in (14, 6, 5, 4, 3)])
        found = pick_sublane(found, wanted & 7)
        at = chunk_base(k) * 2
        for r in range(16):
            send_ans[pl.ds(at + r, 1), :] = found[:, r * 128 : (r + 1) * 128]

    def reply(d):
        pltpu.make_async_remote_copy(
            src_ref=send_ans.at[pl.ds(d * 2, 2), :],
            dst_ref=recv_ans.at[pl.ds(me * 2, 2), :],
            send_sem=send_sem.at[4],
            recv_sem=recv_sem.at[4],
            device_id=(d,),
            device_id_type=MESH,
        ).start()

    for group in (range(0, 5), range(5, 10), range(10, 14), range(14, 16)):
        for k in group:
            answer(k)
        for k in group:
            for j in range(8 if k < 15 else 7):
                reply(chunk_base(k) + inner[j])
    pltpu.make_async_copy(
        send_ans.at[pl.ds(me * 2, 2), :], recv_ans.at[pl.ds(me * 2, 2), :], recv_sem.at[4]
    ).start()
    fid_part = jnp.sum(
        jnp.where(recv_req[...] >= 0, send_ans[...], 0.0), axis=0, keepdims=True
    )
    send_fid[...] = jnp.broadcast_to(fid_part, (8, 128))
    exchange(5, send_fid, recv_fid, 1, 1, lambda d: 0)

    arrived(3, recv_hst, 2)
    norm = jnp.sum(
        jnp.sum(recv_hst[pl.ds(1, 128, stride=2), :], axis=0, keepdims=True), axis=1, keepdims=True
    )
    bins_row = jnp.sum(recv_hst[pl.ds(0, 128, stride=2), :], axis=0, keepdims=True)
    bins_row = 1024.0 * (bins_row / norm)
    bins_row = pltpu.roll(bins_row, lax.rem(128 - lax.rem(me, 16) * 8, 128), 1)
    hist_ref[...] = bins_row[:, :8]

    scale = 4194304.0 / norm
    arrived(4, recv_ans, 2)
    answers = jnp.concatenate(
        [recv_ans[pl.ds(half, 128, stride=2), :] for half in range(2)], axis=1
    )
    answers = jnp.concatenate(split(answers), axis=0)

    def collect(step, c):
        owner = jnp.concatenate([high_ref[pl.ds(step * 8 + k, 1), :] for k in range(8)], axis=1)
        hot = rank_hot[:, pl.ds(pl.multiple_of(step * 1024, 1024), 1024)]
        found = dot(answers, hot)
        found = found[:128] + found[128:]
        found = select_rows(found, [bit_of(owner, p) for p in (6, 5, 4, 3)])
        found = pick_sublane(found, owner & 7) * scale
        for k in range(8):
            probs_ref[pl.ds(step * 8 + k, 1), :] = found[:, k * 128 : (k + 1) * 128]
        return c

    lax.fori_loop(0, 8, collect, 0, unroll=4)

    arrived(5, recv_fid, 1)
    total = jnp.sum(
        jnp.sum(recv_fid[...], axis=0, keepdims=True), axis=1, keepdims=True
    )
    fid_ref[...] = 4194304.0 * (total / norm) / 1048576.0 - 1.0
    sent(0, send_amp, 4)
    sent(1, send_req, 2)
    sent(2, send_wgt, 2)
    sent(3, recv_hst, 2)
    sent(4, send_ans, 2)
    sent(5, recv_fid, 1)


def on_device(state, angles, sample_high, sample_low, marginal_qubits):
    vmem = pl.BlockSpec(memory_space=pltpu.VMEM)
    field = state.reshape(2, 256, 128).transpose(1, 0, 2).reshape(512, 128)
    probs, hist, fid = pl.pallas_call(
        kernel,
        out_shape=(
            jax.ShapeDtypeStruct((64, 128), F32),
            jax.ShapeDtypeStruct((1, 8), F32),
            jax.ShapeDtypeStruct((1, 1), F32),
        ),
        in_specs=[pl.BlockSpec(memory_space=pl.ANY)] * 5,
        out_specs=(vmem, vmem, vmem),
        scratch_shapes=[
            pltpu.VMEM((512, 128), F32),
            pltpu.VMEM((3, 22), F32),
            pltpu.VMEM((64, 128), I32),
            pltpu.VMEM((64, 128), I32),
            pltpu.SMEM((10,), I32),
            pltpu.VMEM((8, 128), F32),
            pltpu.VMEM((8, 24, 128), F32),
            pltpu.VMEM((512, 128), F32),
            pltpu.VMEM((512, 128), F32),
            pltpu.VMEM((256, 128), I32),
            pltpu.VMEM((256, 128), I32),
            pltpu.VMEM((256, 128), F32),
            pltpu.VMEM((256, 128), F32),
            pltpu.VMEM((16, 128), F32),
            pltpu.VMEM((256, 128), F32),
            pltpu.VMEM((256, 128), F32),
            pltpu.VMEM((256, 128), F32),
            pltpu.VMEM((8, 128), F32),
            pltpu.VMEM((128, 128), F32),
            pltpu.VMEM((256, 8192), BF16),
            pltpu.VMEM((64, 128), F32),
            pltpu.VMEM((128, 256), BF16),
            pltpu.VMEM((256, 256), F32),
            pltpu.VMEM((128, 32768), BF16),
            pltpu.VMEM((256, 128), BF16),
            pltpu.SemaphoreType.DMA((6,)),
            pltpu.SemaphoreType.DMA((6,)),
            pltpu.SemaphoreType.DMA((5,)),
        ],
        compiler_params=pltpu.CompilerParams(collective_id=0, has_side_effects=True),
    )(
        field,
        angles.T,
        sample_high.reshape(64, 128),
        sample_low.reshape(64, 128),
        marginal_qubits,
    )
    return probs.reshape(8192), hist.reshape(8), fid.reshape(())


def solution(mesh):
    return jax.shard_map(
        on_device,
        mesh=mesh,
        in_specs=(P(None, "dev"), P(), P("dev", None), P("dev"), P()),
        out_specs=(P("dev"), P("dev"), P()),
        check_vma=False,
    )
```

```python
import functools

import jax
import jax.numpy as jnp
from jax import lax
from jax.experimental import pallas as pl
from jax.experimental.pallas import tpu as pltpu
from jax.sharding import PartitionSpec as P

N = 128
MESH = pl.DeviceIdType.MESH
F32 = jnp.float32
BF16 = jnp.bfloat16
I32 = jnp.int32


def iota(shape, dim):
    return lax.broadcasted_iota(I32, shape, dim)


def dot(a, b):
    return jnp.dot(a, b, preferred_element_type=F32)


def split(x):
    high = x.astype(BF16)
    low = (x - high.astype(F32)).astype(BF16)
    return high, low


def dot3(a, b):
    a_high, a_low = split(a)
    b_high, b_low = split(b)
    return dot(a_high, b_high) + (dot(a_high, b_low) + dot(a_low, b_high))


def complex_mul(a, b):
    return (a[0] * b[0] - a[1] * b[1], a[0] * b[1] + a[1] * b[0])


def gate_entries(angles, trig_ref):
    count = angles.shape[1]
    packed = jnp.concatenate([angles, angles[1:2] + angles[2:3]], axis=0)
    trig_ref[...] = jnp.zeros((8, 128), F32)
    trig_ref[pl.ds(0, 4), pl.ds(0, count)] = jnp.sin(packed)
    trig_ref[pl.ds(4, 4), pl.ds(0, count)] = jnp.cos(packed)
    turned = trig_ref[...].T

    def column(k):
        return jnp.broadcast_to(turned[:24, k : k + 1], (24, 128))

    sin_t, sin_f, sin_l, sin_fl, cos_t, cos_f, cos_l, cos_fl = (column(k) for k in range(8))
    return [
        (cos_t, jnp.zeros_like(cos_t)),
        (-cos_l * sin_t, -sin_l * sin_t),
        (cos_f * sin_t, sin_f * sin_t),
        (cos_fl * cos_t, sin_fl * cos_t),
    ]


def kron_matrix(entry, qubits, transposed):
    size = 2 ** len(qubits)
    lane, sub = iota((8, size), 1), iota((8, size), 0)

    def factor_rows(place, qubit):
        bit = (lane >> place) & 1 == 1

        def choose(zero, one):
            return tuple(
                jnp.where(bit, entry(one, part, qubit, size), entry(zero, part, qubit, size))
                for part in range(2)
            )

        if transposed:
            return choose(0, 2), choose(1, 3)
        return choose(0, 1), choose(2, 3)

    mat = None
    for place, qubit in enumerate(qubits):
        row_zero, row_one = factor_rows(place, qubit)
        if place < 3:
            bit = (sub >> place) & 1 == 1
            factor = tuple(jnp.where(bit, row_one[k], row_zero[k]) for k in range(2))
            mat = factor if mat is None else complex_mul(mat, factor)
        else:
            count = mat[0].shape[0] // 8
            halves = []
            for row in (row_zero, row_one):
                wide = tuple(jnp.concatenate([x] * count, axis=0) for x in row)
                halves.append(complex_mul(mat, wide))
            mat = tuple(jnp.concatenate([halves[0][k], halves[1][k]], axis=0) for k in range(2))
    return mat


def select_rows(values, bits):
    for bit in bits:
        half = values.shape[0] // 2
        values = jnp.where(bit, values[half:], values[:half])
    return values


def pick_sublane(values, index):
    hit = iota(values.shape, 0) == index
    return jnp.sum(jnp.where(hit, values, 0.0), axis=0, keepdims=True)


def one_hot(ids, rows):
    one, zero = jnp.ones(ids.shape, BF16), jnp.zeros(ids.shape, BF16)
    return jnp.concatenate([jnp.where(ids == row, one, zero) for row in rows], axis=1)


def bit_of(x, place):
    return (x >> place) & 1 == 1


def kernel(
    state_hbm, angles_hbm, high_hbm, low_hbm, marg_hbm,
    out_ref,
    state_ref, angles_ref, high_ref, low_ref, marg_ref, trig_ref, gate_ref, send_amp, recv_amp, send_req, recv_req, send_wgt, recv_wgt,
    send_hst, recv_hst, send_ans, recv_ans, send_fid, recv_fid,
    rank_hot, rank_ref, seen_ref, place_ref, want_hot, ids_ref,
    send_sem, recv_sem, load_sem,
):
    me = lax.axis_index("dev")
    loads = [
        pltpu.make_async_copy(src, dst, load_sem.at[k])
        for k, (src, dst) in enumerate(
            [
                (angles_hbm, angles_ref),
                (state_hbm, state_ref),
                (high_hbm, high_ref),
                (low_hbm, low_ref),
                (marg_hbm, marg_ref),
            ]
        )
    ]
    my_z, my_x = me // 32, (me // 8) & 3
    my_y, my_core = (me // 2) & 3, me & 1

    ring = (2, 1, 3, 0)
    z_part = [((my_z + off) & 3) * 32 for off in ring]
    x_part = [((my_x + off) & 3) * 8 for off in ring]
    inner = [((my_y + ring[j // 2]) & 3) * 2 + ((my_core + 1 + j) & 1) for j in range(8)]
    bases = [z_part[k // 4] + x_part[k % 4] for k in range(16)]

    def others(act):
        for k in range(16):
            for j in range(8 if k < 15 else 7):
                act(bases[k] + inner[j])

    for load in loads:
        load.start()
    barrier = pltpu.get_barrier_semaphore()
    others(
        lambda d: pl.semaphore_signal(barrier, inc=1, device_id=(d,), device_id_type=MESH)
    )

    def exchange(which, src, dst, rows, pitch, src_block=None):
        def source(d):
            start = d * pitch if src_block is None else src_block(d)
            return src.at[pl.ds(start, rows), :]

        def send(d):
            pltpu.make_async_remote_copy(
                src_ref=source(d),
                dst_ref=dst.at[pl.ds(me * pitch, rows), :],
                send_sem=send_sem.at[which],
                recv_sem=recv_sem.at[which],
                device_id=(d,),
                device_id_type=MESH,
            ).start()

        others(send)
        pltpu.make_async_copy(
            source(me), dst.at[pl.ds(me * pitch, rows), :], recv_sem.at[which]
        ).start()

    def arrived(which, dst, rows):
        whole = dst.at[pl.ds(0, N * rows), :]
        pltpu.make_async_copy(whole, whole, recv_sem.at[which]).wait()

    def sent(which, dst, rows):
        most = dst.at[pl.ds(0, (N - 1) * rows), :]
        pltpu.make_async_copy(most, most, send_sem.at[which]).wait()

    ids_ref[...] = iota((256, 128), 0).astype(F32).astype(BF16)
    loads[0].wait()
    entries = gate_entries(angles_ref[...], trig_ref)
    for kind in range(4):
        for part in range(2):
            gate_ref[2 * kind + part, :, :] = entries[kind][part]

    def entry(kind, part, qubit, size):
        row = gate_ref[2 * kind + part, pl.ds(qubit, 1), :]
        row = jnp.broadcast_to(row, (8, 128))
        return row if size == 128 else jnp.concatenate([row] * (size // 128), axis=1)

    lane_re, lane_im = kron_matrix(entry, list(range(0, 7)), True)
    row_re, row_im = kron_matrix(entry, list(range(7, 15)), False)
    for load in loads[1:]:
        load.wait()
    field = jnp.concatenate(
        [state_ref[pl.ds(0, 256, stride=2), :], state_ref[pl.ds(1, 256, stride=2), :]], axis=1
    )
    lane_gate = jnp.concatenate(
        [
            jnp.concatenate([lane_re, lane_im], axis=1),
            jnp.concatenate([-lane_im, lane_re], axis=1),
        ],
        axis=0,
    )
    field = dot3(field, lane_gate)
    product = dot3(jnp.concatenate([row_re, row_im], axis=0), field)
    amp_re = product[:256, :128] - product[256:, 128:]
    amp_im = product[:256, 128:] + product[256:, :128]
    for half in range(2):
        send_amp[pl.ds(half, 128, stride=4), :] = amp_re[half * 128 : (half + 1) * 128]
        send_amp[pl.ds(2 + half, 128, stride=4), :] = amp_im[half * 128 : (half + 1) * 128]

    ahead = jnp.where(iota((512, 256), 0) < iota((512, 256), 1), 1.0, 0.0)
    ahead = jnp.where(iota((512, 256), 0) >= 256, 1.0, ahead).astype(BF16)
    seen_ref[...] = jnp.zeros((128, 256), BF16)

    def rank(step, c):
        seen = seen_ref[...]
        rows, hits = [], []
        for sub in range(4):
            at = step * 8 + 2 * sub
            owner = [high_ref[pl.ds(at + half, 1), :] for half in range(2)]
            hot = one_hot(ids_ref[pl.ds(0, 128), :], [x.astype(F32).astype(BF16) for x in owner])
            mine = iota((128, 256), 0) == jnp.concatenate(owner, axis=1)
            rows.append(jnp.concatenate([hot, seen], axis=1))
            hits.append(mine)
            seen = seen + hot
        seen_ref[...] = seen
        counts = dot(jnp.concatenate(rows, axis=0), ahead)
        for sub in range(4):
            ranks = jnp.sum(
                jnp.where(hits[sub], counts[128 * sub : 128 * (sub + 1)], 0.0),
                axis=0,
                keepdims=True,
            )
            for half in range(2):
                rank_ref[pl.ds(step * 8 + 2 * sub + half, 1), :] = ranks[
                    :, half * 128 : (half + 1) * 128
                ]
        return c

    lax.fori_loop(0, 8, rank, 0, unroll=4)
    pl.semaphore_wait(barrier, N - 1)
    exchange(0, send_amp, recv_amp, 4, 4)

    place_ref[...] = jnp.zeros((256, 256), F32)

    def route(step, c):
        lhs_parts, hot_parts = [], []
        ids = ids_ref[...]
        none = jnp.zeros((128, 128), BF16)
        for sub in range(8):
            at = step * 8 + sub
            low = low_ref[pl.ds(at, 1), :]
            low_part = (low & 255).astype(F32).astype(BF16)
            high_part = ((low >> 8) + 1).astype(F32).astype(BF16)
            mine = ids[:128] == high_ref[pl.ds(at, 1), :].astype(F32).astype(BF16)
            ranked = one_hot(ids, [rank_ref[pl.ds(at, 1), :].astype(BF16)])
            rank_hot[:, pl.ds(pl.multiple_of(step * 1024 + sub * 128, 128), 128)] = ranked
            hot_parts.append(ranked)
            lhs_parts.append(
                jnp.concatenate(
                    [jnp.where(mine, low_part, none), jnp.where(mine, high_part, none)], axis=0
                )
            )
        place_ref[...] += lax.dot_general(
            jnp.concatenate(lhs_parts, axis=1),
            jnp.concatenate(hot_parts, axis=1),
            (((1,), (1,)), ((), ())),
            preferred_element_type=F32,
        )
        return c

    lax.fori_loop(0, 8, route, 0, unroll=2)
    asked = (place_ref[:128, :] + 256.0 * (place_ref[128:, :] - 1.0)).astype(I32)
    for half in range(2):
        send_req[pl.ds(half, 128, stride=2), :] = asked[:, half * 128 : (half + 1) * 128]
    exchange(1, send_req, recv_req, 2, 2)

    glob_re, glob_im = kron_matrix(entry, list(range(15, 22)), False)
    glob = jnp.concatenate(
        [
            jnp.concatenate([glob_re, -glob_im], axis=1),
            jnp.concatenate([glob_im, glob_re], axis=1),
        ],
        axis=0,
    )
    bins = iota((1, 1024), 1)
    local_code = jnp.zeros((256, 128), I32)
    global_code = jnp.zeros((128, 128), I32)
    row_id, g_id = iota((256, 128), 0), iota((128, 128), 0)
    local_mask = jnp.int32(0)
    other_mask = jnp.int32(0)
    other_code = jnp.int32(0)
    for k in range(10):
        qubit = marg_ref[k]
        in_lane, in_dev = qubit < 7, (qubit >= 7) & (qubit < 14)
        in_half, in_glob = qubit == 14, qubit >= 15
        place = jnp.where(in_half, 7, jnp.where(in_lane, qubit, 31))
        local_code += ((row_id >> place) & 1) << k
        local_mask += jnp.where(in_lane | in_half, 1 << k, 0)
        g_place = jnp.where(in_glob, qubit - 15, 31)
        global_code += ((g_id >> g_place) & 1) << k
        other_mask += jnp.where(in_glob | in_dev, 1 << k, 0)
        d_place = jnp.where(in_dev, qubit - 7, 31)
        other_code += ((me >> d_place) & 1) << k
    local_code = jnp.concatenate([local_code] * 8, axis=1)
    global_code = jnp.concatenate([global_code + other_code] * 8, axis=1)
    local_hot = jnp.where((bins & local_mask) == local_code, 1.0, 0.0).astype(BF16)
    global_hit = (bins & other_mask) == global_code

    arrived(0, recv_amp, 4)
    parts = [recv_amp[pl.ds(k, 128, stride=4), :] for k in range(4)]
    spread = jnp.concatenate(
        [
            jnp.concatenate([parts[0], parts[1]], axis=1),
            jnp.concatenate([parts[2], parts[3]], axis=1),
        ],
        axis=0,
    )
    final = dot3(glob, spread)
    weight = final[:128] * final[:128] + final[128:] * final[128:]
    for half in range(2):
        send_wgt[pl.ds(half, 128, stride=2), :] = weight[:, half * 128 : (half + 1) * 128]
    exchange(2, send_wgt, recv_wgt, 2, 2)

    folded = dot(jnp.concatenate(split(weight), axis=0), local_hot)
    folded = jnp.where(global_hit, folded[:128] + folded[128:], 0.0)
    partial = jnp.sum(folded, axis=0, keepdims=True)
    norm_part = jnp.sum(weight[:, :128] + weight[:, 128:], axis=0, keepdims=True)
    for row in range(8):
        send_hst[pl.ds(2 * row, 1), :] = partial[:, row * 128 : (row + 1) * 128]
        send_hst[pl.ds(2 * row + 1, 1), :] = norm_part
    exchange(3, send_hst, recv_hst, 2, 2, lambda d: (d // 16) * 2)

    def wanted_of(k):
        at = bases[k] * 2
        return jnp.concatenate([recv_req[pl.ds(at + r, 1), :] for r in range(16)], axis=1)

    arrived(1, recv_req, 2)

    for k in range(16):
        rows = [
            ((recv_req[pl.ds(bases[k] * 2 + r, 1), :] >> 7) & 127).astype(F32).astype(BF16)
            for r in range(16)
        ]
        want_hot[:, pl.ds(k * 2048, 2048)] = one_hot(ids_ref[pl.ds(0, 128), :], rows)

    arrived(2, recv_wgt, 2)
    table = jnp.concatenate(
        [recv_wgt[pl.ds(half, 128, stride=2), :].T for half in range(2)], axis=0
    )
    table = jnp.concatenate(split(table), axis=1)

    def answer(k):
        hot = want_hot[:, pl.ds(k * 2048, 2048)]
        found = dot(table, jnp.concatenate([hot, hot], axis=0))
        wanted = wanted_of(k)
        found = select_rows(found, [bit_of(wanted, p) for p in (14, 6, 5, 4, 3)])
        found = pick_sublane(found, wanted & 7)
        at = bases[k] * 2
        for r in range(16):
            send_ans[pl.ds(at + r, 1), :] = found[:, r * 128 : (r + 1) * 128]

    def reply(d):
        pltpu.make_async_remote_copy(
            src_ref=send_ans.at[pl.ds(d * 2, 2), :],
            dst_ref=recv_ans.at[pl.ds(me * 2, 2), :],
            send_sem=send_sem.at[4],
            recv_sem=recv_sem.at[4],
            device_id=(d,),
            device_id_type=MESH,
        ).start()

    for group in (range(0, 5), range(5, 10), range(10, 14), range(14, 16)):
        for k in group:
            answer(k)
        for k in group:
            for j in range(8 if k < 15 else 7):
                reply(bases[k] + inner[j])
    pltpu.make_async_copy(
        send_ans.at[pl.ds(me * 2, 2), :], recv_ans.at[pl.ds(me * 2, 2), :], recv_sem.at[4]
    ).start()
    fid_part = jnp.sum(
        jnp.where(recv_req[...] >= 0, send_ans[...], 0.0), axis=0, keepdims=True
    )
    send_fid[...] = jnp.broadcast_to(fid_part, (8, 128))
    exchange(5, send_fid, recv_fid, 1, 1, lambda d: 0)

    arrived(3, recv_hst, 2)
    norm = jnp.sum(
        jnp.sum(recv_hst[pl.ds(1, 128, stride=2), :], axis=0, keepdims=True), axis=1, keepdims=True
    )
    bins_row = jnp.sum(recv_hst[pl.ds(0, 128, stride=2), :], axis=0, keepdims=True)
    bins_row = 1024.0 * (bins_row / norm)
    bins_row = pltpu.roll(bins_row, lax.rem(128 - lax.rem(me, 16) * 8, 128), 1)
    out_ref[pl.ds(64, 1), :] = bins_row

    scale = 4194304.0 / norm
    arrived(4, recv_ans, 2)
    answers = jnp.concatenate(
        [recv_ans[pl.ds(half, 128, stride=2), :] for half in range(2)], axis=1
    )
    answers = jnp.concatenate(split(answers), axis=0)

    def collect(step, c):
        owner = jnp.concatenate([high_ref[pl.ds(step * 8 + k, 1), :] for k in range(8)], axis=1)
        hot = rank_hot[:, pl.ds(pl.multiple_of(step * 1024, 1024), 1024)]
        found = dot(answers, hot)
        found = found[:128] + found[128:]
        found = select_rows(found, [bit_of(owner, p) for p in (6, 5, 4, 3)])
        found = pick_sublane(found, owner & 7) * scale
        for k in range(8):
            out_ref[pl.ds(step * 8 + k, 1), :] = found[:, k * 128 : (k + 1) * 128]
        return c

    lax.fori_loop(0, 8, collect, 0, unroll=4)

    arrived(5, recv_fid, 1)
    total = jnp.sum(
        jnp.sum(recv_fid[...], axis=0, keepdims=True), axis=1, keepdims=True
    )
    fidelity = 4194304.0 * (total / norm) / 1048576.0 - 1.0
    out_ref[pl.ds(65, 1), :] = jnp.broadcast_to(fidelity, (1, 128))
    sent(0, send_amp, 4)
    sent(1, send_req, 2)
    sent(2, send_wgt, 2)
    sent(3, recv_hst, 2)
    sent(4, send_ans, 2)
    sent(5, recv_fid, 1)


def unpack(packed_ref, probs_ref, hist_ref, fid_ref):
    probs_ref[...] = packed_ref[pl.ds(0, 64), :]
    hist_ref[...] = packed_ref[pl.ds(64, 1), pl.ds(0, 8)]
    fid_ref[...] = packed_ref[pl.ds(65, 1), pl.ds(0, 1)]


def on_device(state, angles, sample_high, sample_low, marginal_qubits):
    vmem = pl.BlockSpec(memory_space=pltpu.VMEM)
    field = state.reshape(2, 256, 128).transpose(1, 0, 2).reshape(512, 128)
    packed = pl.pallas_call(
        kernel,
        out_shape=jax.ShapeDtypeStruct((72, 128), F32),
        in_specs=[pl.BlockSpec(memory_space=pl.ANY)] * 5,
        out_specs=vmem,
        scratch_shapes=[
            pltpu.VMEM((512, 128), F32),
            pltpu.VMEM((3, 22), F32),
            pltpu.VMEM((64, 128), I32),
            pltpu.VMEM((64, 128), I32),
            pltpu.SMEM((10,), I32),
            pltpu.VMEM((8, 128), F32),
            pltpu.VMEM((8, 24, 128), F32),
            pltpu.VMEM((512, 128), F32),
            pltpu.VMEM((512, 128), F32),
            pltpu.VMEM((256, 128), I32),
            pltpu.VMEM((256, 128), I32),
            pltpu.VMEM((256, 128), F32),
            pltpu.VMEM((256, 128), F32),
            pltpu.VMEM((16, 128), F32),
            pltpu.VMEM((256, 128), F32),
            pltpu.VMEM((256, 128), F32),
            pltpu.VMEM((256, 128), F32),
            pltpu.VMEM((8, 128), F32),
            pltpu.VMEM((128, 128), F32),
            pltpu.VMEM((256, 8192), BF16),
            pltpu.VMEM((64, 128), F32),
            pltpu.VMEM((128, 256), BF16),
            pltpu.VMEM((256, 256), F32),
            pltpu.VMEM((128, 32768), BF16),
            pltpu.VMEM((256, 128), BF16),
            pltpu.SemaphoreType.DMA((6,)),
            pltpu.SemaphoreType.DMA((6,)),
            pltpu.SemaphoreType.DMA((5,)),
        ],
        compiler_params=pltpu.CompilerParams(collective_id=0, has_side_effects=True),
    )(
        field,
        angles.T,
        sample_high.reshape(64, 128),
        sample_low.reshape(64, 128),
        marginal_qubits,
    )
    probs, hist, fid = pl.pallas_call(
        unpack,
        out_shape=(
            jax.ShapeDtypeStruct((64, 128), F32),
            jax.ShapeDtypeStruct((1, 8), F32),
            jax.ShapeDtypeStruct((1, 1), F32),
        ),
        in_specs=[vmem],
        out_specs=(vmem, vmem, vmem),
    )(packed)
    return probs.reshape(8192), hist.reshape(8), fid.reshape(())


def solution(mesh):
    return jax.shard_map(
        on_device,
        mesh=mesh,
        in_specs=(P(None, "dev"), P(), P("dev", None), P("dev"), P()),
        out_specs=(P("dev"), P("dev"), P()),
        check_vma=False,
    )
```

```python
import functools

import jax
import jax.numpy as jnp
from jax import lax
from jax.experimental import pallas as pl
from jax.experimental.pallas import tpu as pltpu
from jax.sharding import PartitionSpec as P

N = 128
MESH = pl.DeviceIdType.MESH
F32 = jnp.float32
BF16 = jnp.bfloat16
I32 = jnp.int32


def iota(shape, dim):
    return lax.broadcasted_iota(I32, shape, dim)


def dot(a, b):
    return jnp.dot(a, b, preferred_element_type=F32)


def split(x):
    high = x.astype(BF16)
    low = (x - high.astype(F32)).astype(BF16)
    return high, low


def dot3(a, b):
    a_high, a_low = split(a)
    b_high, b_low = split(b)
    return dot(a_high, b_high) + (dot(a_high, b_low) + dot(a_low, b_high))


def complex_mul(a, b):
    return (a[0] * b[0] - a[1] * b[1], a[0] * b[1] + a[1] * b[0])


def gate_entries(angles, trig_ref):
    count = angles.shape[1]
    packed = jnp.concatenate([angles, angles[1:2] + angles[2:3]], axis=0)
    trig_ref[...] = jnp.zeros((8, 128), F32)
    trig_ref[pl.ds(0, 4), pl.ds(0, count)] = jnp.sin(packed)
    trig_ref[pl.ds(4, 4), pl.ds(0, count)] = jnp.cos(packed)
    turned = trig_ref[...].T

    def column(k):
        return jnp.broadcast_to(turned[:24, k : k + 1], (24, 128))

    sin_t, sin_f, sin_l, sin_fl, cos_t, cos_f, cos_l, cos_fl = (column(k) for k in range(8))
    return [
        (cos_t, jnp.zeros_like(cos_t)),
        (-cos_l * sin_t, -sin_l * sin_t),
        (cos_f * sin_t, sin_f * sin_t),
        (cos_fl * cos_t, sin_fl * cos_t),
    ]


def kron_matrix(entry, qubits, transposed):
    size = 2 ** len(qubits)
    lane, sub = iota((8, size), 1), iota((8, size), 0)

    def factor_rows(place, qubit):
        bit = (lane >> place) & 1 == 1

        def choose(zero, one):
            return tuple(
                jnp.where(bit, entry(one, part, qubit, size), entry(zero, part, qubit, size))
                for part in range(2)
            )

        if transposed:
            return choose(0, 2), choose(1, 3)
        return choose(0, 1), choose(2, 3)

    mat = None
    for place, qubit in enumerate(qubits):
        row_zero, row_one = factor_rows(place, qubit)
        if place < 3:
            bit = (sub >> place) & 1 == 1
            factor = tuple(jnp.where(bit, row_one[k], row_zero[k]) for k in range(2))
            mat = factor if mat is None else complex_mul(mat, factor)
        else:
            count = mat[0].shape[0] // 8
            halves = []
            for row in (row_zero, row_one):
                wide = tuple(jnp.concatenate([x] * count, axis=0) for x in row)
                halves.append(complex_mul(mat, wide))
            mat = tuple(jnp.concatenate([halves[0][k], halves[1][k]], axis=0) for k in range(2))
    return mat


def select_rows(values, bits):
    for bit in bits:
        half = values.shape[0] // 2
        values = jnp.where(bit, values[half:], values[:half])
    return values


def pick_sublane(values, index):
    hit = iota(values.shape, 0) == index
    return jnp.sum(jnp.where(hit, values, 0.0), axis=0, keepdims=True)


def one_hot(ids, rows):
    one, zero = jnp.ones(ids.shape, BF16), jnp.zeros(ids.shape, BF16)
    return jnp.concatenate([jnp.where(ids == row, one, zero) for row in rows], axis=1)


def bit_of(x, place):
    return (x >> place) & 1 == 1


def kernel(
    state_hbm, angles_hbm, high_hbm, low_hbm, marg_hbm,
    out_ref,
    state_ref, angles_ref, high_ref, low_ref, marg_ref, trig_ref, gate_ref, send_amp, recv_amp, send_req, recv_req, send_wgt, recv_wgt,
    send_hst, recv_hst, send_ans, recv_ans, send_fid, recv_fid,
    rank_hot, rank_ref, seen_ref, place_ref, want_hot, ids_ref,
    send_sem, recv_sem, load_sem,
):
    me = lax.axis_index("dev")
    loads = [
        pltpu.make_async_copy(src, dst, load_sem.at[k])
        for k, (src, dst) in enumerate(
            [
                (angles_hbm, angles_ref),
                (state_hbm, state_ref),
                (high_hbm, high_ref),
                (low_hbm, low_ref),
                (marg_hbm, marg_ref),
            ]
        )
    ]
    my_z, my_x = me // 32, (me // 8) & 3
    my_y, my_core = (me // 2) & 3, me & 1

    ring = (2, 1, 3, 0)
    z_part = [((my_z + off) & 3) * 32 for off in ring]
    x_part = [((my_x + off) & 3) * 8 for off in ring]
    inner = [((my_y + ring[j // 2]) & 3) * 2 + ((my_core + 1 + j) & 1) for j in range(8)]
    bases = [z_part[k // 4] + x_part[k % 4] for k in range(16)]

    def others(act):
        for k in range(16):
            for j in range(8 if k < 15 else 7):
                act(bases[k] + inner[j])

    for load in loads:
        load.start()
    barrier = pltpu.get_barrier_semaphore()
    others(
        lambda d: pl.semaphore_signal(barrier, inc=1, device_id=(d,), device_id_type=MESH)
    )

    def exchange(which, src, dst, rows, pitch, src_block=None):
        def source(d):
            start = d * pitch if src_block is None else src_block(d)
            return src.at[pl.ds(start, rows), :]

        def send(d):
            pltpu.make_async_remote_copy(
                src_ref=source(d),
                dst_ref=dst.at[pl.ds(me * pitch, rows), :],
                send_sem=send_sem.at[which],
                recv_sem=recv_sem.at[which],
                device_id=(d,),
                device_id_type=MESH,
            ).start()

        others(send)
        pltpu.make_async_copy(
            source(me), dst.at[pl.ds(me * pitch, rows), :], recv_sem.at[which]
        ).start()

    def arrived(which, dst, rows):
        whole = dst.at[pl.ds(0, N * rows), :]
        pltpu.make_async_copy(whole, whole, recv_sem.at[which]).wait()

    def sent(which, dst, rows):
        most = dst.at[pl.ds(0, (N - 1) * rows), :]
        pltpu.make_async_copy(most, most, send_sem.at[which]).wait()

    ids_ref[...] = iota((256, 128), 0).astype(F32).astype(BF16)
    loads[0].wait()
    entries = gate_entries(angles_ref[...], trig_ref)
    for kind in range(4):
        for part in range(2):
            gate_ref[2 * kind + part, :, :] = entries[kind][part]

    def entry(kind, part, qubit, size):
        row = gate_ref[2 * kind + part, pl.ds(qubit, 1), :]
        row = jnp.broadcast_to(row, (8, 128))
        return row if size == 128 else jnp.concatenate([row] * (size // 128), axis=1)

    lane_re, lane_im = kron_matrix(entry, list(range(0, 7)), True)
    row_re, row_im = kron_matrix(entry, list(range(7, 15)), False)
    for load in loads[1:]:
        load.wait()
    field = jnp.concatenate(
        [state_ref[pl.ds(0, 256, stride=2), :], state_ref[pl.ds(1, 256, stride=2), :]], axis=1
    )
    lane_gate = jnp.concatenate(
        [
            jnp.concatenate([lane_re, lane_im], axis=1),
            jnp.concatenate([-lane_im, lane_re], axis=1),
        ],
        axis=0,
    )
    field = dot3(field, lane_gate)
    product = dot3(jnp.concatenate([row_re, row_im], axis=0), field)
    amp_re = product[:256, :128] - product[256:, 128:]
    amp_im = product[:256, 128:] + product[256:, :128]
    for half in range(2):
        send_amp[pl.ds(half, 128, stride=4), :] = amp_re[half * 128 : (half + 1) * 128]
        send_amp[pl.ds(2 + half, 128, stride=4), :] = amp_im[half * 128 : (half + 1) * 128]

    ahead = jnp.where(iota((512, 256), 0) < iota((512, 256), 1), 1.0, 0.0)
    ahead = jnp.where(iota((512, 256), 0) >= 256, 1.0, ahead).astype(BF16)
    seen_ref[...] = jnp.zeros((128, 256), BF16)

    def rank(step, c):
        seen = seen_ref[...]
        rows, hits = [], []
        for sub in range(4):
            at = step * 8 + 2 * sub
            owner = [high_ref[pl.ds(at + half, 1), :] for half in range(2)]
            hot = one_hot(ids_ref[pl.ds(0, 128), :], [x.astype(F32).astype(BF16) for x in owner])
            mine = iota((128, 256), 0) == jnp.concatenate(owner, axis=1)
            rows.append(jnp.concatenate([hot, seen], axis=1))
            hits.append(mine)
            seen = seen + hot
        seen_ref[...] = seen
        counts = dot(jnp.concatenate(rows, axis=0), ahead)
        for sub in range(4):
            ranks = jnp.sum(
                jnp.where(hits[sub], counts[128 * sub : 128 * (sub + 1)], 0.0),
                axis=0,
                keepdims=True,
            )
            for half in range(2):
                rank_ref[pl.ds(step * 8 + 2 * sub + half, 1), :] = ranks[
                    :, half * 128 : (half + 1) * 128
                ]
        return c

    lax.fori_loop(0, 8, rank, 0, unroll=4)
    pl.semaphore_wait(barrier, N - 1)
    exchange(0, send_amp, recv_amp, 4, 4)

    place_ref[...] = jnp.zeros((256, 256), F32)

    def route(step, c):
        lhs_parts, hot_parts = [], []
        ids = ids_ref[...]
        none = jnp.zeros((128, 128), BF16)
        for sub in range(8):
            at = step * 8 + sub
            low = low_ref[pl.ds(at, 1), :]
            low_part = (low & 255).astype(F32).astype(BF16)
            high_part = ((low >> 8) + 1).astype(F32).astype(BF16)
            mine = ids[:128] == high_ref[pl.ds(at, 1), :].astype(F32).astype(BF16)
            ranked = one_hot(ids, [rank_ref[pl.ds(at, 1), :].astype(BF16)])
            rank_hot[:, pl.ds(pl.multiple_of(step * 1024 + sub * 128, 128), 128)] = ranked
            hot_parts.append(ranked)
            lhs_parts.append(
                jnp.concatenate(
                    [jnp.where(mine, low_part, none), jnp.where(mine, high_part, none)], axis=0
                )
            )
        place_ref[...] += lax.dot_general(
            jnp.concatenate(lhs_parts, axis=1),
            jnp.concatenate(hot_parts, axis=1),
            (((1,), (1,)), ((), ())),
            preferred_element_type=F32,
        )
        return c

    lax.fori_loop(0, 8, route, 0, unroll=2)
    asked = (place_ref[:128, :] + 256.0 * (place_ref[128:, :] - 1.0)).astype(I32)
    for half in range(2):
        send_req[pl.ds(half, 128, stride=2), :] = asked[:, half * 128 : (half + 1) * 128]
    exchange(1, send_req, recv_req, 2, 2)

    glob_re, glob_im = kron_matrix(entry, list(range(15, 22)), False)
    glob = jnp.concatenate(
        [
            jnp.concatenate([glob_re, -glob_im], axis=1),
            jnp.concatenate([glob_im, glob_re], axis=1),
        ],
        axis=0,
    )
    bins = iota((1, 1024), 1)
    local_code = jnp.zeros((256, 128), I32)
    global_code = jnp.zeros((128, 128), I32)
    row_id, g_id = iota((256, 128), 0), iota((128, 128), 0)
    local_mask = jnp.int32(0)
    other_mask = jnp.int32(0)
    other_code = jnp.int32(0)
    for k in range(10):
        qubit = marg_ref[k]
        in_lane, in_dev = qubit < 7, (qubit >= 7) & (qubit < 14)
        in_half, in_glob = qubit == 14, qubit >= 15
        place = jnp.where(in_half, 7, jnp.where(in_lane, qubit, 31))
        local_code += ((row_id >> place) & 1) << k
        local_mask += jnp.where(in_lane | in_half, 1 << k, 0)
        g_place = jnp.where(in_glob, qubit - 15, 31)
        global_code += ((g_id >> g_place) & 1) << k
        other_mask += jnp.where(in_glob | in_dev, 1 << k, 0)
        d_place = jnp.where(in_dev, qubit - 7, 31)
        other_code += ((me >> d_place) & 1) << k
    local_code = jnp.concatenate([local_code] * 8, axis=1)
    global_code = jnp.concatenate([global_code + other_code] * 8, axis=1)
    local_hot = jnp.where((bins & local_mask) == local_code, 1.0, 0.0).astype(BF16)
    global_hit = (bins & other_mask) == global_code

    arrived(0, recv_amp, 4)
    parts = [recv_amp[pl.ds(k, 128, stride=4), :] for k in range(4)]
    spread = jnp.concatenate(
        [
            jnp.concatenate([parts[0], parts[1]], axis=1),
            jnp.concatenate([parts[2], parts[3]], axis=1),
        ],
        axis=0,
    )
    final = dot3(glob, spread)
    weight = final[:128] * final[:128] + final[128:] * final[128:]
    for half in range(2):
        send_wgt[pl.ds(half, 128, stride=2), :] = weight[:, half * 128 : (half + 1) * 128]
    exchange(2, send_wgt, recv_wgt, 2, 2)

    folded = dot(jnp.concatenate(split(weight), axis=0), local_hot)
    folded = jnp.where(global_hit, folded[:128] + folded[128:], 0.0)
    partial = jnp.sum(folded, axis=0, keepdims=True)
    norm_part = jnp.sum(weight[:, :128] + weight[:, 128:], axis=0, keepdims=True)
    for row in range(8):
        send_hst[pl.ds(2 * row, 1), :] = partial[:, row * 128 : (row + 1) * 128]
        send_hst[pl.ds(2 * row + 1, 1), :] = norm_part
    exchange(3, send_hst, recv_hst, 2, 2, lambda d: (d // 16) * 2)

    def wanted_of(k):
        at = bases[k] * 2
        return jnp.concatenate([recv_req[pl.ds(at + r, 1), :] for r in range(16)], axis=1)

    arrived(1, recv_req, 2)

    for k in range(16):
        rows = [
            ((recv_req[pl.ds(bases[k] * 2 + r, 1), :] >> 7) & 127).astype(F32).astype(BF16)
            for r in range(16)
        ]
        want_hot[:, pl.ds(k * 2048, 2048)] = one_hot(ids_ref[pl.ds(0, 128), :], rows)

    arrived(2, recv_wgt, 2)
    table = jnp.concatenate(
        [recv_wgt[pl.ds(half, 128, stride=2), :].T for half in range(2)], axis=0
    )
    table = jnp.concatenate(split(table), axis=1)

    def answer(k):
        hot = want_hot[:, pl.ds(k * 2048, 2048)]
        found = dot(table, jnp.concatenate([hot, hot], axis=0))
        wanted = wanted_of(k)
        found = select_rows(found, [bit_of(wanted, p) for p in (14, 6, 5, 4, 3)])
        found = pick_sublane(found, wanted & 7)
        at = bases[k] * 2
        for r in range(16):
            send_ans[pl.ds(at + r, 1), :] = found[:, r * 128 : (r + 1) * 128]

    def reply(d):
        pltpu.make_async_remote_copy(
            src_ref=send_ans.at[pl.ds(d * 2, 2), :],
            dst_ref=recv_ans.at[pl.ds(me * 2, 2), :],
            send_sem=send_sem.at[4],
            recv_sem=recv_sem.at[4],
            device_id=(d,),
            device_id_type=MESH,
        ).start()

    for group in (range(0,6),range(6,12),range(12,15),range(15,16)):
        for k in group:
            answer(k)
        for k in group:
            for j in range(8 if k < 15 else 7):
                reply(bases[k] + inner[j])
    pltpu.make_async_copy(
        send_ans.at[pl.ds(me * 2, 2), :], recv_ans.at[pl.ds(me * 2, 2), :], recv_sem.at[4]
    ).start()
    fid_part = jnp.sum(
        jnp.where(recv_req[...] >= 0, send_ans[...], 0.0), axis=0, keepdims=True
    )
    send_fid[...] = jnp.broadcast_to(fid_part, (8, 128))
    exchange(5, send_fid, recv_fid, 1, 1, lambda d: 0)

    arrived(3, recv_hst, 2)
    norm = jnp.sum(
        jnp.sum(recv_hst[pl.ds(1, 128, stride=2), :], axis=0, keepdims=True), axis=1, keepdims=True
    )
    bins_row = jnp.sum(recv_hst[pl.ds(0, 128, stride=2), :], axis=0, keepdims=True)
    bins_row = 1024.0 * (bins_row / norm)
    bins_row = pltpu.roll(bins_row, lax.rem(128 - lax.rem(me, 16) * 8, 128), 1)
    out_ref[pl.ds(64, 1), :] = bins_row

    scale = 4194304.0 / norm
    arrived(4, recv_ans, 2)
    answers = jnp.concatenate(
        [recv_ans[pl.ds(half, 128, stride=2), :] for half in range(2)], axis=1
    )
    answers = jnp.concatenate(split(answers), axis=0)

    def collect(step, c):
        owner = jnp.concatenate([high_ref[pl.ds(step * 8 + k, 1), :] for k in range(8)], axis=1)
        hot = rank_hot[:, pl.ds(pl.multiple_of(step * 1024, 1024), 1024)]
        found = dot(answers, hot)
        found = found[:128] + found[128:]
        found = select_rows(found, [bit_of(owner, p) for p in (6, 5, 4, 3)])
        found = pick_sublane(found, owner & 7) * scale
        for k in range(8):
            out_ref[pl.ds(step * 8 + k, 1), :] = found[:, k * 128 : (k + 1) * 128]
        return c

    lax.fori_loop(0, 8, collect, 0, unroll=4)

    arrived(5, recv_fid, 1)
    total = jnp.sum(
        jnp.sum(recv_fid[...], axis=0, keepdims=True), axis=1, keepdims=True
    )
    fidelity = 4194304.0 * (total / norm) / 1048576.0 - 1.0
    out_ref[pl.ds(65, 1), :] = jnp.broadcast_to(fidelity, (1, 128))
    sent(0, send_amp, 4)
    sent(1, send_req, 2)
    sent(2, send_wgt, 2)
    sent(3, recv_hst, 2)
    sent(4, send_ans, 2)
    sent(5, recv_fid, 1)


def unpack(packed_ref, probs_ref, hist_ref, fid_ref):
    probs_ref[...] = packed_ref[pl.ds(0, 64), :]
    hist_ref[...] = packed_ref[pl.ds(64, 1), pl.ds(0, 8)]
    fid_ref[...] = packed_ref[pl.ds(65, 1), pl.ds(0, 1)]


def on_device(state, angles, sample_high, sample_low, marginal_qubits):
    vmem = pl.BlockSpec(memory_space=pltpu.VMEM)
    field = state.reshape(2, 256, 128).transpose(1, 0, 2).reshape(512, 128)
    operands = (
        field,
        angles.T,
        sample_high.reshape(64, 128),
        sample_low.reshape(64, 128),
        marginal_qubits,
    )
    packed = pl.pallas_call(
        kernel,
        out_shape=jax.ShapeDtypeStruct((72, 128), F32),
        in_specs=[pl.BlockSpec(memory_space=pl.ANY)] * 5,
        out_specs=vmem,
        scratch_shapes=[
            pltpu.VMEM((512, 128), F32),
            pltpu.VMEM((3, 22), F32),
            pltpu.VMEM((64, 128), I32),
            pltpu.VMEM((64, 128), I32),
            pltpu.SMEM((10,), I32),
            pltpu.VMEM((8, 128), F32),
            pltpu.VMEM((8, 24, 128), F32),
            pltpu.VMEM((512, 128), F32),
            pltpu.VMEM((512, 128), F32),
            pltpu.VMEM((256, 128), I32),
            pltpu.VMEM((256, 128), I32),
            pltpu.VMEM((256, 128), F32),
            pltpu.VMEM((256, 128), F32),
            pltpu.VMEM((16, 128), F32),
            pltpu.VMEM((256, 128), F32),
            pltpu.VMEM((256, 128), F32),
            pltpu.VMEM((256, 128), F32),
            pltpu.VMEM((8, 128), F32),
            pltpu.VMEM((128, 128), F32),
            pltpu.VMEM((256, 8192), BF16),
            pltpu.VMEM((64, 128), F32),
            pltpu.VMEM((128, 256), BF16),
            pltpu.VMEM((256, 256), F32),
            pltpu.VMEM((128, 32768), BF16),
            pltpu.VMEM((256, 128), BF16),
            pltpu.SemaphoreType.DMA((6,)),
            pltpu.SemaphoreType.DMA((6,)),
            pltpu.SemaphoreType.DMA((5,)),
        ],
        compiler_params=pltpu.CompilerParams(
            collective_id=0, has_side_effects=True, vmem_limit_bytes=40 * 1024 * 1024
        ),
    )(*(pltpu.with_memory_space_constraint(x, pltpu.HBM) for x in operands))
    probs, hist, fid = pl.pallas_call(
        unpack,
        out_shape=(
            jax.ShapeDtypeStruct((64, 128), F32),
            jax.ShapeDtypeStruct((1, 8), F32),
            jax.ShapeDtypeStruct((1, 1), F32),
        ),
        in_specs=[vmem],
        out_specs=(vmem, vmem, vmem),
        compiler_params=pltpu.CompilerParams(vmem_limit_bytes=8 * 1024 * 1024),
    )(packed)
    return probs.reshape(8192), hist.reshape(8), fid.reshape(())


def solution(mesh):
    return jax.shard_map(
        on_device,
        mesh=mesh,
        in_specs=(P(None, "dev"), P(), P("dev", None), P("dev"), P()),
        out_specs=(P("dev"), P("dev"), P()),
        check_vma=False,
    )
```

```python
import functools

import jax
import jax.numpy as jnp
from jax import lax
from jax.experimental import pallas as pl
from jax.experimental.pallas import tpu as pltpu
from jax.sharding import PartitionSpec as P

N = 128
MESH = pl.DeviceIdType.MESH
F32 = jnp.float32
BF16 = jnp.bfloat16
I32 = jnp.int32


def iota(shape, dim):
    return lax.broadcasted_iota(I32, shape, dim)


def dot(a, b):
    return jnp.dot(a, b, preferred_element_type=F32)


def split(x):
    high = x.astype(BF16)
    low = (x - high.astype(F32)).astype(BF16)
    return high, low


def dot3(a, b):
    a_high, a_low = split(a)
    b_high, b_low = split(b)
    return dot(a_high, b_high) + (dot(a_high, b_low) + dot(a_low, b_high))


def complex_mul(a, b):
    return (a[0] * b[0] - a[1] * b[1], a[0] * b[1] + a[1] * b[0])


def gate_entries(angles, trig_ref):
    count = angles.shape[1]
    packed = jnp.concatenate([angles, angles[1:2] + angles[2:3]], axis=0)
    trig_ref[...] = jnp.zeros((8, 128), F32)
    trig_ref[pl.ds(0, 4), pl.ds(0, count)] = jnp.sin(packed)
    trig_ref[pl.ds(4, 4), pl.ds(0, count)] = jnp.cos(packed)
    turned = trig_ref[...].T

    def column(k):
        return jnp.broadcast_to(turned[:24, k : k + 1], (24, 128))

    sin_t, sin_f, sin_l, sin_fl, cos_t, cos_f, cos_l, cos_fl = (column(k) for k in range(8))
    return [
        (cos_t, jnp.zeros_like(cos_t)),
        (-cos_l * sin_t, -sin_l * sin_t),
        (cos_f * sin_t, sin_f * sin_t),
        (cos_fl * cos_t, sin_fl * cos_t),
    ]


def kron_matrix(entry, qubits, transposed):
    size = 2 ** len(qubits)
    lane, sub = iota((8, size), 1), iota((8, size), 0)

    def factor_rows(place, qubit):
        bit = (lane >> place) & 1 == 1

        def choose(zero, one):
            return tuple(
                jnp.where(bit, entry(one, part, qubit, size), entry(zero, part, qubit, size))
                for part in range(2)
            )

        if transposed:
            return choose(0, 2), choose(1, 3)
        return choose(0, 1), choose(2, 3)

    mat = None
    for place, qubit in enumerate(qubits):
        row_zero, row_one = factor_rows(place, qubit)
        if place < 3:
            bit = (sub >> place) & 1 == 1
            factor = tuple(jnp.where(bit, row_one[k], row_zero[k]) for k in range(2))
            mat = factor if mat is None else complex_mul(mat, factor)
        else:
            count = mat[0].shape[0] // 8
            halves = []
            for row in (row_zero, row_one):
                wide = tuple(jnp.concatenate([x] * count, axis=0) for x in row)
                halves.append(complex_mul(mat, wide))
            mat = tuple(jnp.concatenate([halves[0][k], halves[1][k]], axis=0) for k in range(2))
    return mat


def select_rows(values, bits):
    for bit in bits:
        half = values.shape[0] // 2
        values = jnp.where(bit, values[half:], values[:half])
    return values


def pick_sublane(values, index):
    hit = iota(values.shape, 0) == index
    return jnp.sum(jnp.where(hit, values, 0.0), axis=0, keepdims=True)


def one_hot(ids, rows):
    one, zero = jnp.ones(ids.shape, BF16), jnp.zeros(ids.shape, BF16)
    return jnp.concatenate([jnp.where(ids == row, one, zero) for row in rows], axis=1)


def bit_of(x, place):
    return (x >> place) & 1 == 1


def kernel(
    state_hbm, angles_hbm, high_hbm, low_hbm, marg_hbm,
    out_ref,
    state_ref, angles_ref, high_ref, low_ref, marg_ref, trig_ref, gate_ref, send_amp, recv_amp, send_req, recv_req, send_wgt, recv_wgt,
    send_hst, recv_hst, send_ans, recv_ans, send_fid, recv_fid,
    rank_hot, rank_ref, seen_ref, place_ref, want_hot, ids_ref,
    send_sem, recv_sem, load_sem,
):
    me = lax.axis_index("dev")
    loads = [
        pltpu.make_async_copy(src, dst, load_sem.at[k])
        for k, (src, dst) in enumerate(
            [
                (angles_hbm, angles_ref),
                (state_hbm, state_ref),
                (high_hbm, high_ref),
                (low_hbm, low_ref),
                (marg_hbm, marg_ref),
            ]
        )
    ]
    my_z, my_x = me // 32, (me // 8) & 3
    my_y, my_core = (me // 2) & 3, me & 1

    ring = (2, 1, 3, 0)
    z_part = [((my_z + off) & 3) * 32 for off in ring]
    x_part = [((my_x + off) & 3) * 8 for off in ring]
    inner = [((my_y + ring[j // 2]) & 3) * 2 + ((my_core + 1 + j) & 1) for j in range(8)]
    bases = [z_part[k // 4] + x_part[k % 4] for k in range(16)]

    def others(act):
        for k in range(16):
            for j in range(8 if k < 15 else 7):
                act(bases[k] + inner[j])

    for load in loads:
        load.start()
    barrier = pltpu.get_barrier_semaphore()
    others(
        lambda d: pl.semaphore_signal(barrier, inc=1, device_id=(d,), device_id_type=MESH)
    )

    def exchange(which, src, dst, rows, pitch, src_block=None):
        def source(d):
            start = d * pitch if src_block is None else src_block(d)
            return src.at[pl.ds(start, rows), :]

        def send(d):
            pltpu.make_async_remote_copy(
                src_ref=source(d),
                dst_ref=dst.at[pl.ds(me * pitch, rows), :],
                send_sem=send_sem.at[which],
                recv_sem=recv_sem.at[which],
                device_id=(d,),
                device_id_type=MESH,
            ).start()

        others(send)
        pltpu.make_async_copy(
            source(me), dst.at[pl.ds(me * pitch, rows), :], recv_sem.at[which]
        ).start()

    def arrived(which, dst, rows):
        whole = dst.at[pl.ds(0, N * rows), :]
        pltpu.make_async_copy(whole, whole, recv_sem.at[which]).wait()

    def sent(which, dst, rows):
        most = dst.at[pl.ds(0, (N - 1) * rows), :]
        pltpu.make_async_copy(most, most, send_sem.at[which]).wait()

    ids_ref[...] = iota((256, 128), 0).astype(F32).astype(BF16)
    loads[0].wait()
    entries = gate_entries(angles_ref[...], trig_ref)
    for kind in range(4):
        for part in range(2):
            gate_ref[2 * kind + part, :, :] = entries[kind][part]

    def entry(kind, part, qubit, size):
        row = gate_ref[2 * kind + part, pl.ds(qubit, 1), :]
        row = jnp.broadcast_to(row, (8, 128))
        return row if size == 128 else jnp.concatenate([row] * (size // 128), axis=1)

    lane_re, lane_im = kron_matrix(entry, list(range(0, 7)), True)
    row_re, row_im = kron_matrix(entry, list(range(7, 15)), False)
    for load in loads[1:]:
        load.wait()
    field = jnp.concatenate(
        [state_ref[pl.ds(0, 256, stride=2), :], state_ref[pl.ds(1, 256, stride=2), :]], axis=1
    )
    lane_gate = jnp.concatenate(
        [
            jnp.concatenate([lane_re, lane_im], axis=1),
            jnp.concatenate([-lane_im, lane_re], axis=1),
        ],
        axis=0,
    )
    field = dot3(field, lane_gate)
    product = dot3(jnp.concatenate([row_re, row_im], axis=0), field)
    amp_re = product[:256, :128] - product[256:, 128:]
    amp_im = product[:256, 128:] + product[256:, :128]
    for half in range(2):
        send_amp[pl.ds(half, 128, stride=4), :] = amp_re[half * 128 : (half + 1) * 128]
        send_amp[pl.ds(2 + half, 128, stride=4), :] = amp_im[half * 128 : (half + 1) * 128]

    ahead = jnp.where(iota((512, 256), 0) < iota((512, 256), 1), 1.0, 0.0)
    ahead = jnp.where(iota((512, 256), 0) >= 256, 1.0, ahead).astype(BF16)
    seen_ref[...] = jnp.zeros((128, 256), BF16)

    def rank(step, c):
        seen = seen_ref[...]
        rows, hits = [], []
        for sub in range(4):
            at = step * 8 + 2 * sub
            owner = [high_ref[pl.ds(at + half, 1), :] for half in range(2)]
            hot = one_hot(ids_ref[pl.ds(0, 128), :], [x.astype(F32).astype(BF16) for x in owner])
            mine = iota((128, 256), 0) == jnp.concatenate(owner, axis=1)
            rows.append(jnp.concatenate([hot, seen], axis=1))
            hits.append(mine)
            seen = seen + hot
        seen_ref[...] = seen
        counts = dot(jnp.concatenate(rows, axis=0), ahead)
        for sub in range(4):
            ranks = jnp.sum(
                jnp.where(hits[sub], counts[128 * sub : 128 * (sub + 1)], 0.0),
                axis=0,
                keepdims=True,
            )
            for half in range(2):
                rank_ref[pl.ds(step * 8 + 2 * sub + half, 1), :] = ranks[
                    :, half * 128 : (half + 1) * 128
                ]
        return c

    lax.fori_loop(0, 8, rank, 0, unroll=4)
    pl.semaphore_wait(barrier, N - 1)
    exchange(0, send_amp, recv_amp, 4, 4)

    place_ref[...] = jnp.zeros((256, 256), F32)

    def route(step, c):
        lhs_parts, hot_parts = [], []
        ids = ids_ref[...]
        none = jnp.zeros((128, 128), BF16)
        for sub in range(8):
            at = step * 8 + sub
            low = low_ref[pl.ds(at, 1), :]
            low_part = (low & 255).astype(F32).astype(BF16)
            high_part = ((low >> 8) + 1).astype(F32).astype(BF16)
            mine = ids[:128] == high_ref[pl.ds(at, 1), :].astype(F32).astype(BF16)
            ranked = one_hot(ids, [rank_ref[pl.ds(at, 1), :].astype(BF16)])
            rank_hot[:, pl.ds(pl.multiple_of(step * 1024 + sub * 128, 128), 128)] = ranked
            hot_parts.append(ranked)
            lhs_parts.append(
                jnp.concatenate(
                    [jnp.where(mine, low_part, none), jnp.where(mine, high_part, none)], axis=0
                )
            )
        place_ref[...] += lax.dot_general(
            jnp.concatenate(lhs_parts, axis=1),
            jnp.concatenate(hot_parts, axis=1),
            (((1,), (1,)), ((), ())),
            preferred_element_type=F32,
        )
        return c

    lax.fori_loop(0, 8, route, 0, unroll=2)
    asked = (place_ref[:128, :] + 256.0 * (place_ref[128:, :] - 1.0)).astype(I32)
    for half in range(2):
        send_req[pl.ds(half, 128, stride=2), :] = asked[:, half * 128 : (half + 1) * 128]
    exchange(1, send_req, recv_req, 2, 2)

    glob_re, glob_im = kron_matrix(entry, list(range(15, 22)), False)
    glob = jnp.concatenate(
        [
            jnp.concatenate([glob_re, -glob_im], axis=1),
            jnp.concatenate([glob_im, glob_re], axis=1),
        ],
        axis=0,
    )
    bins = iota((1, 1024), 1)
    local_code = jnp.zeros((256, 128), I32)
    global_code = jnp.zeros((128, 128), I32)
    row_id, g_id = iota((256, 128), 0), iota((128, 128), 0)
    local_mask = jnp.int32(0)
    other_mask = jnp.int32(0)
    other_code = jnp.int32(0)
    for k in range(10):
        qubit = marg_ref[k]
        in_lane, in_dev = qubit < 7, (qubit >= 7) & (qubit < 14)
        in_half, in_glob = qubit == 14, qubit >= 15
        place = jnp.where(in_half, 7, jnp.where(in_lane, qubit, 31))
        local_code += ((row_id >> place) & 1) << k
        local_mask += jnp.where(in_lane | in_half, 1 << k, 0)
        g_place = jnp.where(in_glob, qubit - 15, 31)
        global_code += ((g_id >> g_place) & 1) << k
        other_mask += jnp.where(in_glob | in_dev, 1 << k, 0)
        d_place = jnp.where(in_dev, qubit - 7, 31)
        other_code += ((me >> d_place) & 1) << k
    local_code = jnp.concatenate([local_code] * 8, axis=1)
    global_code = jnp.concatenate([global_code + other_code] * 8, axis=1)
    local_hot = jnp.where((bins & local_mask) == local_code, 1.0, 0.0).astype(BF16)
    global_hit = (bins & other_mask) == global_code

    arrived(0, recv_amp, 4)
    parts = [recv_amp[pl.ds(k, 128, stride=4), :] for k in range(4)]
    spread = jnp.concatenate(
        [
            jnp.concatenate([parts[0], parts[1]], axis=1),
            jnp.concatenate([parts[2], parts[3]], axis=1),
        ],
        axis=0,
    )
    final = dot3(glob, spread)
    weight = final[:128] * final[:128] + final[128:] * final[128:]
    for half in range(2):
        send_wgt[pl.ds(half, 128, stride=2), :] = weight[:, half * 128 : (half + 1) * 128]
    exchange(2, send_wgt, recv_wgt, 2, 2)

    folded = dot(jnp.concatenate(split(weight), axis=0), local_hot)
    folded = jnp.where(global_hit, folded[:128] + folded[128:], 0.0)
    partial = jnp.sum(folded, axis=0, keepdims=True)
    norm_part = jnp.sum(weight[:, :128] + weight[:, 128:], axis=0, keepdims=True)
    for row in range(8):
        send_hst[pl.ds(2 * row, 1), :] = partial[:, row * 128 : (row + 1) * 128]
        send_hst[pl.ds(2 * row + 1, 1), :] = norm_part
    exchange(3, send_hst, recv_hst, 2, 2, lambda d: (d // 16) * 2)

    def wanted_of(k):
        at = bases[k] * 2
        return jnp.concatenate([recv_req[pl.ds(at + r, 1), :] for r in range(16)], axis=1)

    arrived(1, recv_req, 2)

    for k in range(16):
        rows = [
            ((recv_req[pl.ds(bases[k] * 2 + r, 1), :] >> 7) & 127).astype(F32).astype(BF16)
            for r in range(16)
        ]
        want_hot[:, pl.ds(k * 2048, 2048)] = one_hot(ids_ref[pl.ds(0, 128), :], rows)

    arrived(2, recv_wgt, 2)
    table = jnp.concatenate(
        [recv_wgt[pl.ds(half, 128, stride=2), :].T for half in range(2)], axis=0
    )
    table = jnp.concatenate(split(table), axis=1)

    def answer(k):
        hot = want_hot[:, pl.ds(k * 2048, 2048)]
        found = dot(table, jnp.concatenate([hot, hot], axis=0))
        wanted = wanted_of(k)
        found = select_rows(found, [bit_of(wanted, p) for p in (14, 6, 5, 4, 3)])
        found = pick_sublane(found, wanted & 7)
        at = bases[k] * 2
        for r in range(16):
            send_ans[pl.ds(at + r, 1), :] = found[:, r * 128 : (r + 1) * 128]

    def reply(d):
        pltpu.make_async_remote_copy(
            src_ref=send_ans.at[pl.ds(d * 2, 2), :],
            dst_ref=recv_ans.at[pl.ds(me * 2, 2), :],
            send_sem=send_sem.at[4],
            recv_sem=recv_sem.at[4],
            device_id=(d,),
            device_id_type=MESH,
        ).start()

    for group in (range(0, 5), range(5, 9), range(9, 12), range(12, 14), range(14, 15), range(15, 16)):
        for k in group:
            answer(k)
        for k in group:
            for j in range(8 if k < 15 else 7):
                reply(bases[k] + inner[j])
    pltpu.make_async_copy(
        send_ans.at[pl.ds(me * 2, 2), :], recv_ans.at[pl.ds(me * 2, 2), :], recv_sem.at[4]
    ).start()
    fid_part = jnp.sum(
        jnp.where(recv_req[...] >= 0, send_ans[...], 0.0), axis=0, keepdims=True
    )
    send_fid[...] = jnp.broadcast_to(fid_part, (8, 128))
    exchange(5, send_fid, recv_fid, 1, 1, lambda d: 0)

    arrived(3, recv_hst, 2)
    norm = jnp.sum(
        jnp.sum(recv_hst[pl.ds(1, 128, stride=2), :], axis=0, keepdims=True), axis=1, keepdims=True
    )
    bins_row = jnp.sum(recv_hst[pl.ds(0, 128, stride=2), :], axis=0, keepdims=True)
    bins_row = 1024.0 * (bins_row / norm)
    bins_row = pltpu.roll(bins_row, lax.rem(128 - lax.rem(me, 16) * 8, 128), 1)
    out_ref[pl.ds(64, 1), :] = bins_row

    scale = 4194304.0 / norm
    arrived(4, recv_ans, 2)
    answers = jnp.concatenate(
        [recv_ans[pl.ds(half, 128, stride=2), :] for half in range(2)], axis=1
    )
    answers = jnp.concatenate(split(answers), axis=0)

    def collect(step, c):
        owner = jnp.concatenate([high_ref[pl.ds(step * 8 + k, 1), :] for k in range(8)], axis=1)
        hot = rank_hot[:, pl.ds(pl.multiple_of(step * 1024, 1024), 1024)]
        found = dot(answers, hot)
        found = found[:128] + found[128:]
        found = select_rows(found, [bit_of(owner, p) for p in (6, 5, 4, 3)])
        found = pick_sublane(found, owner & 7) * scale
        for k in range(8):
            out_ref[pl.ds(step * 8 + k, 1), :] = found[:, k * 128 : (k + 1) * 128]
        return c

    lax.fori_loop(0, 8, collect, 0, unroll=8)

    arrived(5, recv_fid, 1)
    total = jnp.sum(
        jnp.sum(recv_fid[...], axis=0, keepdims=True), axis=1, keepdims=True
    )
    fidelity = 4194304.0 * (total / norm) / 1048576.0 - 1.0
    out_ref[pl.ds(65, 1), :] = jnp.broadcast_to(fidelity, (1, 128))
    sent(0, send_amp, 4)
    sent(1, send_req, 2)
    sent(2, send_wgt, 2)
    sent(3, recv_hst, 2)
    sent(4, send_ans, 2)
    sent(5, recv_fid, 1)


def unpack(packed_ref, probs_hbm, hist_ref, fid_ref, sem):
    probs = pltpu.make_async_copy(packed_ref.at[pl.ds(0, 64), :], probs_hbm, sem)
    probs.start()
    hist_ref[...] = packed_ref[pl.ds(64, 1), pl.ds(0, 8)]
    fid_ref[...] = packed_ref[pl.ds(65, 1), pl.ds(0, 1)]
    probs.wait()


def on_device(state, angles, sample_high, sample_low, marginal_qubits):
    vmem = pl.BlockSpec(memory_space=pltpu.VMEM)
    field = state.reshape(2, 256, 128).transpose(1, 0, 2).reshape(512, 128)
    operands = (
        field,
        angles.T,
        sample_high.reshape(64, 128),
        sample_low.reshape(64, 128),
        marginal_qubits,
    )
    packed = pl.pallas_call(
        kernel,
        out_shape=jax.ShapeDtypeStruct((72, 128), F32),
        in_specs=[pl.BlockSpec(memory_space=pl.ANY)] * 5,
        out_specs=vmem,
        scratch_shapes=[
            pltpu.VMEM((512, 128), F32),
            pltpu.VMEM((3, 22), F32),
            pltpu.VMEM((64, 128), I32),
            pltpu.VMEM((64, 128), I32),
            pltpu.SMEM((10,), I32),
            pltpu.VMEM((8, 128), F32),
            pltpu.VMEM((8, 24, 128), F32),
            pltpu.VMEM((512, 128), F32),
            pltpu.VMEM((512, 128), F32),
            pltpu.VMEM((256, 128), I32),
            pltpu.VMEM((256, 128), I32),
            pltpu.VMEM((256, 128), F32),
            pltpu.VMEM((256, 128), F32),
            pltpu.VMEM((16, 128), F32),
            pltpu.VMEM((256, 128), F32),
            pltpu.VMEM((256, 128), F32),
            pltpu.VMEM((256, 128), F32),
            pltpu.VMEM((8, 128), F32),
            pltpu.VMEM((128, 128), F32),
            pltpu.VMEM((256, 8192), BF16),
            pltpu.VMEM((64, 128), F32),
            pltpu.VMEM((128, 256), BF16),
            pltpu.VMEM((256, 256), F32),
            pltpu.VMEM((128, 32768), BF16),
            pltpu.VMEM((256, 128), BF16),
            pltpu.SemaphoreType.DMA((6,)),
            pltpu.SemaphoreType.DMA((6,)),
            pltpu.SemaphoreType.DMA((5,)),
        ],
        compiler_params=pltpu.CompilerParams(
            collective_id=0, has_side_effects=True, vmem_limit_bytes=40 * 1024 * 1024
        ),
    )(*(pltpu.with_memory_space_constraint(x, pltpu.HBM) for x in operands))
    probs, hist, fid = pl.pallas_call(
        unpack,
        out_shape=(
            jax.ShapeDtypeStruct((64, 128), F32),
            jax.ShapeDtypeStruct((1, 8), F32),
            jax.ShapeDtypeStruct((1, 1), F32),
        ),
        in_specs=[vmem],
        out_specs=(pl.BlockSpec(memory_space=pl.ANY), vmem, vmem),
        scratch_shapes=[pltpu.SemaphoreType.DMA],
        compiler_params=pltpu.CompilerParams(vmem_limit_bytes=8 * 1024 * 1024),
    )(packed)
    return probs.reshape(8192), hist.reshape(8), fid.reshape(())


def solution(mesh):
    return jax.shard_map(
        on_device,
        mesh=mesh,
        in_specs=(P(None, "dev"), P(), P("dev", None), P("dev"), P()),
        out_specs=(P("dev"), P("dev"), P()),
        check_vma=False,
    )
```

```python
import functools

import jax
import jax.numpy as jnp
from jax import lax
from jax.experimental import pallas as pl
from jax.experimental.pallas import tpu as pltpu
from jax.sharding import PartitionSpec as P

N = 128
MESH = pl.DeviceIdType.MESH
F32 = jnp.float32
BF16 = jnp.bfloat16
I32 = jnp.int32


def iota(shape, dim):
    return lax.broadcasted_iota(I32, shape, dim)


def dot(a, b):
    return jnp.dot(a, b, preferred_element_type=F32)


def split(x):
    high = x.astype(BF16)
    low = (x - high.astype(F32)).astype(BF16)
    return high, low


def dot3(a, b):
    a_high, a_low = split(a)
    b_high, b_low = split(b)
    return dot(a_high, b_high) + (dot(a_high, b_low) + dot(a_low, b_high))


def complex_mul(a, b):
    return (a[0] * b[0] - a[1] * b[1], a[0] * b[1] + a[1] * b[0])


def gate_entries(angles, trig_ref):
    count = angles.shape[1]
    packed = jnp.concatenate([angles, angles[1:2] + angles[2:3]], axis=0)
    trig_ref[...] = jnp.zeros((8, 128), F32)
    trig_ref[pl.ds(0, 4), pl.ds(0, count)] = jnp.sin(packed)
    trig_ref[pl.ds(4, 4), pl.ds(0, count)] = jnp.cos(packed)
    turned = trig_ref[...].T

    def column(k):
        return jnp.broadcast_to(turned[:24, k : k + 1], (24, 128))

    sin_t, sin_f, sin_l, sin_fl, cos_t, cos_f, cos_l, cos_fl = (column(k) for k in range(8))
    return [
        (cos_t, jnp.zeros_like(cos_t)),
        (-cos_l * sin_t, -sin_l * sin_t),
        (cos_f * sin_t, sin_f * sin_t),
        (cos_fl * cos_t, sin_fl * cos_t),
    ]


def kron_matrix(entry, qubits, transposed):
    size = 2 ** len(qubits)
    lane, sub = iota((8, size), 1), iota((8, size), 0)

    def factor_rows(place, qubit):
        bit = (lane >> place) & 1 == 1

        def choose(zero, one):
            return tuple(
                jnp.where(bit, entry(one, part, qubit, size), entry(zero, part, qubit, size))
                for part in range(2)
            )

        if transposed:
            return choose(0, 2), choose(1, 3)
        return choose(0, 1), choose(2, 3)

    mat = None
    for place, qubit in enumerate(qubits):
        row_zero, row_one = factor_rows(place, qubit)
        if place < 3:
            bit = (sub >> place) & 1 == 1
            factor = tuple(jnp.where(bit, row_one[k], row_zero[k]) for k in range(2))
            mat = factor if mat is None else complex_mul(mat, factor)
        else:
            count = mat[0].shape[0] // 8
            halves = []
            for row in (row_zero, row_one):
                wide = tuple(jnp.concatenate([x] * count, axis=0) for x in row)
                halves.append(complex_mul(mat, wide))
            mat = tuple(jnp.concatenate([halves[0][k], halves[1][k]], axis=0) for k in range(2))
    return mat


def select_rows(values, bits):
    for bit in bits:
        half = values.shape[0] // 2
        values = jnp.where(bit, values[half:], values[:half])
    return values


def pick_sublane(values, index):
    hit = iota(values.shape, 0) == index
    return jnp.sum(jnp.where(hit, values, 0.0), axis=0, keepdims=True)


def one_hot(ids, rows):
    one, zero = jnp.ones(ids.shape, BF16), jnp.zeros(ids.shape, BF16)
    return jnp.concatenate([jnp.where(ids == row, one, zero) for row in rows], axis=1)


def bit_of(x, place):
    return (x >> place) & 1 == 1


def kernel(
    state_hbm, angles_hbm, high_hbm, low_hbm, marg_hbm,
    out_ref,
    state_ref, angles_ref, high_ref, low_ref, marg_ref, trig_ref, gate_ref, send_amp, recv_amp, send_req, recv_req, send_wgt, recv_wgt,
    send_hst, recv_hst, send_ans, recv_ans, send_fid, recv_fid,
    rank_hot, rank_ref, seen_ref, place_ref, want_hot, ids_ref,
    send_sem, recv_sem, load_sem,
):
    me = lax.axis_index("dev")
    loads = [
        pltpu.make_async_copy(src, dst, load_sem.at[k])
        for k, (src, dst) in enumerate(
            [
                (angles_hbm, angles_ref),
                (state_hbm, state_ref),
                (high_hbm, high_ref),
                (low_hbm, low_ref),
                (marg_hbm, marg_ref),
            ]
        )
    ]
    my_z, my_x = me // 32, (me // 8) & 3
    my_y, my_core = (me // 2) & 3, me & 1

    ring = (2, 1, 3, 0)
    z_part = [((my_z + off) & 3) * 32 for off in ring]
    x_part = [((my_x + off) & 3) * 8 for off in ring]
    inner = [((my_y + ring[j // 2]) & 3) * 2 + ((1 + j + my_core * (j // 6)) & 1) for j in range(8)]
    bases = [z_part[k // 4] + x_part[k % 4] for k in range(16)]

    def others(act):
        for k in range(16):
            for j in range(8 if k < 15 else 7):
                act(bases[k] + inner[j])

    for load in loads:
        load.start()
    barrier = pltpu.get_barrier_semaphore()
    others(
        lambda d: pl.semaphore_signal(barrier, inc=1, device_id=(d,), device_id_type=MESH)
    )

    def exchange(which, src, dst, rows, pitch, src_block=None):
        def source(d):
            start = d * pitch if src_block is None else src_block(d)
            return src.at[pl.ds(start, rows), :]

        def send(d):
            pltpu.make_async_remote_copy(
                src_ref=source(d),
                dst_ref=dst.at[pl.ds(me * pitch, rows), :],
                send_sem=send_sem.at[which],
                recv_sem=recv_sem.at[which],
                device_id=(d,),
                device_id_type=MESH,
            ).start()

        others(send)
        pltpu.make_async_copy(
            source(me), dst.at[pl.ds(me * pitch, rows), :], recv_sem.at[which]
        ).start()

    def arrived(which, dst, rows):
        whole = dst.at[pl.ds(0, N * rows), :]
        pltpu.make_async_copy(whole, whole, recv_sem.at[which]).wait()

    def sent(which, dst, rows):
        most = dst.at[pl.ds(0, (N - 1) * rows), :]
        pltpu.make_async_copy(most, most, send_sem.at[which]).wait()

    ids_ref[...] = iota((256, 128), 0).astype(F32).astype(BF16)
    loads[0].wait()
    entries = gate_entries(angles_ref[...], trig_ref)
    for kind in range(4):
        for part in range(2):
            gate_ref[2 * kind + part, :, :] = entries[kind][part]

    def entry(kind, part, qubit, size):
        row = gate_ref[2 * kind + part, pl.ds(qubit, 1), :]
        row = jnp.broadcast_to(row, (8, 128))
        return row if size == 128 else jnp.concatenate([row] * (size // 128), axis=1)

    lane_re, lane_im = kron_matrix(entry, list(range(0, 7)), True)
    row_re, row_im = kron_matrix(entry, list(range(7, 15)), False)
    for load in loads[1:]:
        load.wait()
    field = jnp.concatenate(
        [state_ref[pl.ds(0, 256, stride=2), :], state_ref[pl.ds(1, 256, stride=2), :]], axis=1
    )
    lane_gate = jnp.concatenate(
        [
            jnp.concatenate([lane_re, lane_im], axis=1),
            jnp.concatenate([-lane_im, lane_re], axis=1),
        ],
        axis=0,
    )
    field = dot3(field, lane_gate)
    product = dot3(jnp.concatenate([row_re, row_im], axis=0), field)
    amp_re = product[:256, :128] - product[256:, 128:]
    amp_im = product[:256, 128:] + product[256:, :128]
    for half in range(2):
        send_amp[pl.ds(half, 128, stride=4), :] = amp_re[half * 128 : (half + 1) * 128]
        send_amp[pl.ds(2 + half, 128, stride=4), :] = amp_im[half * 128 : (half + 1) * 128]

    ahead = jnp.where(iota((512, 256), 0) < iota((512, 256), 1), 1.0, 0.0)
    ahead = jnp.where(iota((512, 256), 0) >= 256, 1.0, ahead).astype(BF16)
    seen_ref[...] = jnp.zeros((128, 256), BF16)

    def rank(step, c):
        seen = seen_ref[...]
        rows, hits = [], []
        for sub in range(4):
            at = step * 8 + 2 * sub
            owner = [high_ref[pl.ds(at + half, 1), :] for half in range(2)]
            hot = one_hot(ids_ref[pl.ds(0, 128), :], [x.astype(F32).astype(BF16) for x in owner])
            mine = iota((128, 256), 0) == jnp.concatenate(owner, axis=1)
            rows.append(jnp.concatenate([hot, seen], axis=1))
            hits.append(mine)
            seen = seen + hot
        seen_ref[...] = seen
        counts = dot(jnp.concatenate(rows, axis=0), ahead)
        for sub in range(4):
            ranks = jnp.sum(
                jnp.where(hits[sub], counts[128 * sub : 128 * (sub + 1)], 0.0),
                axis=0,
                keepdims=True,
            )
            for half in range(2):
                rank_ref[pl.ds(step * 8 + 2 * sub + half, 1), :] = ranks[
                    :, half * 128 : (half + 1) * 128
                ]
        return c

    lax.fori_loop(0, 8, rank, 0, unroll=4)
    pl.semaphore_wait(barrier, N - 1)
    exchange(0, send_amp, recv_amp, 4, 4)

    place_ref[...] = jnp.zeros((256, 256), F32)

    def route(step, c):
        lhs_parts, hot_parts = [], []
        ids = ids_ref[...]
        none = jnp.zeros((128, 128), BF16)
        for sub in range(8):
            at = step * 8 + sub
            low = low_ref[pl.ds(at, 1), :]
            low_part = (low & 255).astype(F32).astype(BF16)
            high_part = ((low >> 8) + 1).astype(F32).astype(BF16)
            mine = ids[:128] == high_ref[pl.ds(at, 1), :].astype(F32).astype(BF16)
            ranked = one_hot(ids, [rank_ref[pl.ds(at, 1), :].astype(BF16)])
            rank_hot[:, pl.ds(pl.multiple_of(step * 1024 + sub * 128, 128), 128)] = ranked
            hot_parts.append(ranked)
            lhs_parts.append(
                jnp.concatenate(
                    [jnp.where(mine, low_part, none), jnp.where(mine, high_part, none)], axis=0
                )
            )
        place_ref[...] += lax.dot_general(
            jnp.concatenate(lhs_parts, axis=1),
            jnp.concatenate(hot_parts, axis=1),
            (((1,), (1,)), ((), ())),
            preferred_element_type=F32,
        )
        return c

    lax.fori_loop(0, 8, route, 0, unroll=2)
    asked = (place_ref[:128, :] + 256.0 * (place_ref[128:, :] - 1.0)).astype(I32)
    for half in range(2):
        send_req[pl.ds(half, 128, stride=2), :] = asked[:, half * 128 : (half + 1) * 128]
    exchange(1, send_req, recv_req, 2, 2)

    glob_re, glob_im = kron_matrix(entry, list(range(15, 22)), False)
    glob = jnp.concatenate(
        [
            jnp.concatenate([glob_re, -glob_im], axis=1),
            jnp.concatenate([glob_im, glob_re], axis=1),
        ],
        axis=0,
    )
    bins = iota((1, 1024), 1)
    local_code = jnp.zeros((256, 128), I32)
    global_code = jnp.zeros((128, 128), I32)
    row_id, g_id = iota((256, 128), 0), iota((128, 128), 0)
    local_mask = jnp.int32(0)
    other_mask = jnp.int32(0)
    other_code = jnp.int32(0)
    for k in range(10):
        qubit = marg_ref[k]
        in_lane, in_dev = qubit < 7, (qubit >= 7) & (qubit < 14)
        in_half, in_glob = qubit == 14, qubit >= 15
        place = jnp.where(in_half, 7, jnp.where(in_lane, qubit, 31))
        local_code += ((row_id >> place) & 1) << k
        local_mask += jnp.where(in_lane | in_half, 1 << k, 0)
        g_place = jnp.where(in_glob, qubit - 15, 31)
        global_code += ((g_id >> g_place) & 1) << k
        other_mask += jnp.where(in_glob | in_dev, 1 << k, 0)
        d_place = jnp.where(in_dev, qubit - 7, 31)
        other_code += ((me >> d_place) & 1) << k
    local_code = jnp.concatenate([local_code] * 8, axis=1)
    global_code = jnp.concatenate([global_code + other_code] * 8, axis=1)
    local_hot = jnp.where((bins & local_mask) == local_code, 1.0, 0.0).astype(BF16)
    global_hit = (bins & other_mask) == global_code

    arrived(0, recv_amp, 4)
    parts = [recv_amp[pl.ds(k, 128, stride=4), :] for k in range(4)]
    spread = jnp.concatenate(
        [
            jnp.concatenate([parts[0], parts[1]], axis=1),
            jnp.concatenate([parts[2], parts[3]], axis=1),
        ],
        axis=0,
    )
    final = dot3(glob, spread)
    weight = final[:128] * final[:128] + final[128:] * final[128:]
    for half in range(2):
        send_wgt[pl.ds(half, 128, stride=2), :] = weight[:, half * 128 : (half + 1) * 128]
    exchange(2, send_wgt, recv_wgt, 2, 2)

    folded = dot(jnp.concatenate(split(weight), axis=0), local_hot)
    folded = jnp.where(global_hit, folded[:128] + folded[128:], 0.0)
    partial = jnp.sum(folded, axis=0, keepdims=True)
    norm_part = jnp.sum(weight[:, :128] + weight[:, 128:], axis=0, keepdims=True)
    for row in range(8):
        send_hst[pl.ds(2 * row, 1), :] = partial[:, row * 128 : (row + 1) * 128]
        send_hst[pl.ds(2 * row + 1, 1), :] = norm_part
    exchange(3, send_hst, recv_hst, 2, 2, lambda d: (d // 16) * 2)

    def wanted_of(k):
        at = bases[k] * 2
        return jnp.concatenate([recv_req[pl.ds(at + r, 1), :] for r in range(16)], axis=1)

    arrived(1, recv_req, 2)

    for k in range(16):
        rows = [
            ((recv_req[pl.ds(bases[k] * 2 + r, 1), :] >> 7) & 127).astype(F32).astype(BF16)
            for r in range(16)
        ]
        want_hot[:, pl.ds(k * 2048, 2048)] = one_hot(ids_ref[pl.ds(0, 128), :], rows)

    arrived(2, recv_wgt, 2)
    table = jnp.concatenate(
        [recv_wgt[pl.ds(half, 128, stride=2), :].T for half in range(2)], axis=0
    )
    table = jnp.concatenate(split(table), axis=1)

    def answer(k):
        hot = want_hot[:, pl.ds(k * 2048, 2048)]
        found = dot(table, jnp.concatenate([hot, hot], axis=0))
        wanted = wanted_of(k)
        found = select_rows(found, [bit_of(wanted, p) for p in (14, 6, 5, 4, 3)])
        found = pick_sublane(found, wanted & 7)
        at = bases[k] * 2
        for r in range(16):
            send_ans[pl.ds(at + r, 1), :] = found[:, r * 128 : (r + 1) * 128]

    def reply(d):
        pltpu.make_async_remote_copy(
            src_ref=send_ans.at[pl.ds(d * 2, 2), :],
            dst_ref=recv_ans.at[pl.ds(me * 2, 2), :],
            send_sem=send_sem.at[4],
            recv_sem=recv_sem.at[4],
            device_id=(d,),
            device_id_type=MESH,
        ).start()

    for group in (range(0,6),range(6,12),range(12,15),range(15,16)):
        for k in group:
            answer(k)
        for k in group:
            for j in range(8 if k < 15 else 7):
                reply(bases[k] + inner[j])
    pltpu.make_async_copy(
        send_ans.at[pl.ds(me * 2, 2), :], recv_ans.at[pl.ds(me * 2, 2), :], recv_sem.at[4]
    ).start()
    fid_part = jnp.sum(
        jnp.where(recv_req[...] >= 0, send_ans[...], 0.0), axis=0, keepdims=True
    )
    send_fid[...] = jnp.broadcast_to(fid_part, (8, 128))
    exchange(5, send_fid, recv_fid, 1, 1, lambda d: 0)

    arrived(3, recv_hst, 2)
    norm = jnp.sum(
        jnp.sum(recv_hst[pl.ds(1, 128, stride=2), :], axis=0, keepdims=True), axis=1, keepdims=True
    )
    bins_row = jnp.sum(recv_hst[pl.ds(0, 128, stride=2), :], axis=0, keepdims=True)
    bins_row = 1024.0 * (bins_row / norm)
    bins_row = pltpu.roll(bins_row, lax.rem(128 - lax.rem(me, 16) * 8, 128), 1)
    out_ref[pl.ds(64, 1), :] = bins_row

    scale = 4194304.0 / norm
    arrived(4, recv_ans, 2)
    answers = jnp.concatenate(
        [recv_ans[pl.ds(half, 128, stride=2), :] for half in range(2)], axis=1
    )
    answers = jnp.concatenate(split(answers), axis=0)

    def collect(step, c):
        owner = jnp.concatenate([high_ref[pl.ds(step * 8 + k, 1), :] for k in range(8)], axis=1)
        hot = rank_hot[:, pl.ds(pl.multiple_of(step * 1024, 1024), 1024)]
        found = dot(answers, hot)
        found = found[:128] + found[128:]
        found = select_rows(found, [bit_of(owner, p) for p in (6, 5, 4, 3)])
        found = pick_sublane(found, owner & 7) * scale
        for k in range(8):
            out_ref[pl.ds(step * 8 + k, 1), :] = found[:, k * 128 : (k + 1) * 128]
        return c

    lax.fori_loop(0, 8, collect, 0, unroll=4)

    arrived(5, recv_fid, 1)
    total = jnp.sum(
        jnp.sum(recv_fid[...], axis=0, keepdims=True), axis=1, keepdims=True
    )
    fidelity = 4194304.0 * (total / norm) / 1048576.0 - 1.0
    out_ref[pl.ds(65, 1), :] = jnp.broadcast_to(fidelity, (1, 128))
    sent(0, send_amp, 4)
    sent(1, send_req, 2)
    sent(2, send_wgt, 2)
    sent(3, recv_hst, 2)
    sent(4, send_ans, 2)
    sent(5, recv_fid, 1)


def unpack(packed_ref, probs_ref, hist_ref, fid_ref):
    probs_ref[...] = packed_ref[pl.ds(0, 64), :]
    hist_ref[...] = packed_ref[pl.ds(64, 1), pl.ds(0, 8)]
    fid_ref[...] = packed_ref[pl.ds(65, 1), pl.ds(0, 1)]


def on_device(state, angles, sample_high, sample_low, marginal_qubits):
    vmem = pl.BlockSpec(memory_space=pltpu.VMEM)
    field = state.reshape(2, 256, 128).transpose(1, 0, 2).reshape(512, 128)
    operands = (
        field,
        angles.T,
        sample_high.reshape(64, 128),
        sample_low.reshape(64, 128),
        marginal_qubits,
    )
    packed = pl.pallas_call(
        kernel,
        out_shape=jax.ShapeDtypeStruct((72, 128), F32),
        in_specs=[pl.BlockSpec(memory_space=pl.ANY)] * 5,
        out_specs=vmem,
        scratch_shapes=[
            pltpu.VMEM((512, 128), F32),
            pltpu.VMEM((3, 22), F32),
            pltpu.VMEM((64, 128), I32),
            pltpu.VMEM((64, 128), I32),
            pltpu.SMEM((10,), I32),
            pltpu.VMEM((8, 128), F32),
            pltpu.VMEM((8, 24, 128), F32),
            pltpu.VMEM((512, 128), F32),
            pltpu.VMEM((512, 128), F32),
            pltpu.VMEM((256, 128), I32),
            pltpu.VMEM((256, 128), I32),
            pltpu.VMEM((256, 128), F32),
            pltpu.VMEM((256, 128), F32),
            pltpu.VMEM((16, 128), F32),
            pltpu.VMEM((256, 128), F32),
            pltpu.VMEM((256, 128), F32),
            pltpu.VMEM((256, 128), F32),
            pltpu.VMEM((8, 128), F32),
            pltpu.VMEM((128, 128), F32),
            pltpu.VMEM((256, 8192), BF16),
            pltpu.VMEM((64, 128), F32),
            pltpu.VMEM((128, 256), BF16),
            pltpu.VMEM((256, 256), F32),
            pltpu.VMEM((128, 32768), BF16),
            pltpu.VMEM((256, 128), BF16),
            pltpu.SemaphoreType.DMA((6,)),
            pltpu.SemaphoreType.DMA((6,)),
            pltpu.SemaphoreType.DMA((5,)),
        ],
        compiler_params=pltpu.CompilerParams(
            collective_id=0, has_side_effects=True, vmem_limit_bytes=40 * 1024 * 1024
        ),
    )(*(pltpu.with_memory_space_constraint(x, pltpu.HBM) for x in operands))
    probs, hist, fid = pl.pallas_call(
        unpack,
        out_shape=(
            jax.ShapeDtypeStruct((64, 128), F32),
            jax.ShapeDtypeStruct((1, 8), F32),
            jax.ShapeDtypeStruct((1, 1), F32),
        ),
        in_specs=[vmem],
        out_specs=(vmem, vmem, vmem),
        compiler_params=pltpu.CompilerParams(vmem_limit_bytes=8 * 1024 * 1024),
    )(packed)
    return probs.reshape(8192), hist.reshape(8), fid.reshape(())


def solution(mesh):
    return jax.shard_map(
        on_device,
        mesh=mesh,
        in_specs=(P(None, "dev"), P(), P("dev", None), P("dev"), P()),
        out_specs=(P("dev"), P("dev"), P()),
        check_vma=False,
    )
```
